32 devices in a mesh: fsdp: 8 (over y, x, core), tensor: 4 (over z).
Axes of the slice: x: 2, y: 2, z: 4, core: 2. Of those that a mesh axis runs over, the one named last changes fastest.
Arguments:
- block_input: bfloat16 [8192, 2048], P(('fsdp', 'tensor')), may hold values from -6 to 6
- doc_ids: int32 [8, 1024], P('fsdp'), may hold values from 0 to 5, never falling along the last dimension, each value on 1 to 512 neighbouring positions
- w_query: bfloat16 [1, 2048, 2048], P(None, 'fsdp', 'tensor')
- w_keyval: bfloat16 [1, 2048, 8, 128], P(None, 'fsdp', 'tensor')
- w_attn_out: bfloat16 [1, 2048, 2048], P(None, 'tensor', 'fsdp'), may hold values from -0.5 to 0.5
- w_gate_up: bfloat16 [1, 2048, 2, 8192], P(None, 'fsdp', None, 'tensor'), may hold values from -0.125 to 0.125
- w_down: bfloat16 [1, 8192, 2048], P(None, 'tensor', 'fsdp'), may hold values from -0.0625 to 0.0625
- norm_gains: bfloat16 [1, 2, 2048], P(None, None, 'fsdp'), may hold values from 0.5 to 1.5
- out_cotangent: float32 [8192, 2048], P(('fsdp', 'tensor')), may hold values from -6 to 6
Outputs:
- block_output: float32 [8192, 2048], P(('fsdp', 'tensor'))
- grad_input: float32 [8192, 2048], P(('fsdp', 'tensor'))
- grad_w_query: float32 [1, 2048, 2048], P(None, 'fsdp', 'tensor')
- grad_w_keyval: float32 [1, 2048, 8, 128], P(None, 'fsdp', 'tensor')
- grad_w_attn_out: float32 [1, 2048, 2048], P(None, 'tensor', 'fsdp')
- grad_w_gate_up: float32 [1, 2048, 2, 8192], P(None, 'fsdp', None, 'tensor')
- grad_w_down: float32 [1, 8192, 2048], P(None, 'tensor', 'fsdp')
- grad_norm_gains: float32 [1, 2, 2048], P(None, None, 'fsdp')
The draws below stay inside these ranges and needn't reach their ends.
Inputs may be any that keep to these rules, and one draw needn't show every extreme that they name: `doc_ids`: in each row document numbers never fall, every number of 0 to 5 appears, each document holds 1 to 512 tokens and one holds exactly 512.
All inputs are finite; a program needn't handle non-finite values.
Results may differ from the reference program's by a relative error of at most 0.014.
Values may be sent and summed in bfloat16 or wider, within the bound.
A program may use at most 320 MiB of HBM per device.

```python
import math
import jax
import jax.numpy as jnp
import numpy as np
from jax import lax

D = 2048
HQ = 32
KVH = 8
HD = 64
FF = 8192
LAYERS = 1
TOK_FS = 1024
MAXLEN = 512
DOCS = 6
SHARDS = 8
TOKENS = 8192


def attention_pair(key):
    key_pair, key_query = jax.random.split(jax.random.fold_in(key, 11), 2)
    keyval = jax.random.normal(key_pair, (LAYERS, D, KVH, 2 * HD), jnp.float32) * D ** (-0.5)
    query_table = jax.random.normal(key_query, (LAYERS, D, KVH, HQ // KVH, HD), jnp.float32) * D ** (-0.5)
    return (query_table.reshape(LAYERS, D, HQ * HD), keyval)


def draw_w_query(key, part):
    return attention_pair(key)[0].astype(jnp.bfloat16)


def draw_w_keyval(key, part):
    return attention_pair(key)[1].astype(jnp.bfloat16)


def strengthened(entries, rng, source, target, blocks, factor):
    def block_of(dim):
        return (jnp.arange(entries.shape[dim]) // (entries.shape[dim] // blocks)).reshape((-1,) + (1,) * (entries.ndim - 1 - dim))

    near = jax.random.permutation(rng, blocks)[block_of(target)]
    second = (block_of(target) + blocks // 2) % blocks
    return jnp.where((block_of(source) == near) | (block_of(source) == second), factor * entries, entries)


def block_scale(key, extent, cuts, low, top_value):
    def one(position, blocks):
        steps = jax.random.uniform(jax.random.fold_in(jax.random.fold_in(key, 6), position), (blocks,), jnp.float32, low / len(cuts), top_value / len(cuts))
        return jnp.repeat(jnp.exp(steps), extent[position] // blocks).reshape((-1,) + (1,) * (len(extent) - position - 1))

    factor_of = one(*cuts[0])
    for cut in cuts[1:]:
        factor_of = factor_of * one(*cut)
    return factor_of


def profile(amount, total, most, lean):
    weights = [(1 << 20) // math.isqrt(grade ** lean) + 1 for grade in range(2, amount + 1)]
    spare, given = total - most - (amount - 1), [1] * (amount - 1)
    while spare > 0:
        candidates = [i for i in range(amount - 1) if given[i] < most]
        whole, left = sum([weights[i] for i in candidates]), spare
        for i in candidates:
            more = min(most - given[i], max(1, left * weights[i] // whole), spare)
            given[i] = given[i] + more
            spare = spare - more
    return np.array([most] + given)


def ragged_sizes(stream_key, count, total, limit, slope):
    if count == 2:
        one = jax.random.randint(stream_key, (), max(1, total - limit), min(limit, total - 1) + 1)
        return jnp.stack([one, total - one])
    lengths = jnp.asarray(profile(count, total, limit, slope), jnp.int32)
    twos = (count - 1) // 2
    source_of, receiver = lengths[1:1 + 2 * twos:2], lengths[2:2 + 2 * twos:2]
    room = jnp.minimum(source_of - 1, limit - receiver)
    shifted = jax.random.randint(jax.random.fold_in(stream_key, 1), (twos,), 0, 1 << 20) % (room + 1)
    lengths = lengths.at[1:1 + 2 * twos:2].set(source_of - shifted).at[2:2 + 2 * twos:2].set(receiver + shifted)
    return lengths[jax.random.permutation(jax.random.fold_in(stream_key, 2), count)]


def centred(rng, shape, spread, limit, cuts=(), kind=jnp.bfloat16):
    level = block_scale(rng, shape, cuts, -0.22, 0.18) if cuts else 1.0
    entries = jax.random.normal(rng, shape, jnp.float32) * spread * level
    return jnp.minimum(jnp.maximum(entries, -limit), limit).astype(kind)


def heavy_noise(own_key, dims, width, bound, pieces, heavy, kind=jnp.bfloat16):
    result = width * jax.random.normal(own_key, dims, jnp.float32)
    if pieces:
        result = result * block_scale(own_key, dims, pieces, -0.22, 0.18)
    return jnp.clip(strengthened(result, jax.random.fold_in(own_key, 3), *heavy), -bound, bound).astype(kind)


def setup_inputs(seed: int = 0) -> dict:
    arg_keys = jax.random.split(jax.random.key(seed), 10)
    return {
        "block_input": heavy_noise(arg_keys[0], (TOKENS, D), 1.0, 6.0, ((0, 32),), (0, 1, 32, 2.75)),
        "doc_ids": jax.vmap(lambda own: jnp.searchsorted(jnp.cumsum(ragged_sizes(own, DOCS, TOK_FS, MAXLEN, 2)), jnp.arange(TOK_FS), side="right"))(jax.random.split(arg_keys[1], SHARDS)).reshape((SHARDS, TOK_FS)).astype(jnp.int32),
        "w_query": draw_w_query(jax.random.fold_in(arg_keys[9], 71), 0),
        "w_keyval": draw_w_keyval(jax.random.fold_in(arg_keys[9], 71), 0),
        "w_attn_out": centred(arg_keys[4], (LAYERS, HQ * HD, D), (HQ * HD // 16) ** -0.5, 0.5, ((1, 4), (2, 8))),
        "w_gate_up": centred(arg_keys[5], (LAYERS, D, 2, FF), D ** -0.5, 0.125, ((1, 8), (3, 4))),
        "w_down": centred(arg_keys[6], (LAYERS, FF, D), FF ** -0.5, 0.0625, ((1, 4), (2, 8))),
        "norm_gains": jnp.clip(1.0 + 0.1 * jax.random.normal(arg_keys[7], (LAYERS, 2, D), jnp.float32), 0.5, 1.5).astype(jnp.bfloat16),
        "out_cotangent": heavy_noise(arg_keys[8], (TOKENS, D), 1.0, 6.0, ((0, 32),), (0, 1, 32, 2.75), jnp.float32),
    }


NORM_EPSILON = 1e-05
ROPE_BASE = 500000.0

def as_wide(array_in):
    return lax.optimization_barrier(array_in).astype(jnp.float32)

def norm_apply(residual, gain):
    inverse = lax.rsqrt(lax.optimization_barrier(jnp.mean(residual * residual, axis=-1, keepdims=True)) + NORM_EPSILON)
    return (inverse, (residual * inverse * gain.astype(jnp.float32)).astype(jnp.bfloat16))

def norm_back(residual, inverse, gain, grad_normed):
    scaled = grad_normed * gain.astype(jnp.float32)
    grad_gain = lax.optimization_barrier(jnp.sum(grad_normed * residual * inverse, axis=0))
    grad_residual = inverse * scaled - residual * inverse * inverse * inverse * lax.optimization_barrier(jnp.mean(scaled * residual, axis=-1, keepdims=True))
    return (grad_residual, grad_gain)

def rope_tables(doc_row, head_size):
    places = jnp.arange(doc_row.shape[0], dtype=jnp.int32)
    doc_start = jnp.concatenate([jnp.array([True]), doc_row[1:] != doc_row[:-1]])
    starts = lax.cummax(jnp.where(doc_start, places, 0).astype(jnp.int32), axis=0)
    exponent = jnp.arange(head_size // 2, dtype=jnp.float32) * (-2.0 / head_size)
    angles = (places - starts).astype(jnp.float32)[:, None] * jnp.power(ROPE_BASE, exponent)[None, :]
    return (jnp.cos(angles), jnp.sin(angles))

def rotate(vectors, cosine, sine_table, direction_sign):
    half_size = vectors.shape[-1] // 2
    table_shape = (vectors.shape[0],) + (1,) * (vectors.ndim - 2) + (half_size,)
    cos_part = cosine.reshape(table_shape)
    sin_part = direction_sign * sine_table.reshape(table_shape)
    first_half = vectors[..., :half_size]
    second = vectors[..., half_size:]
    return jnp.concatenate([first_half * cos_part - second * sin_part, second * cos_part + first_half * sin_part], axis=-1)

def block_mask(doc_row, block_start, block_rows, key_low, key_high):
    places = jnp.arange(doc_row.shape[0], dtype=jnp.int32)
    own_docs = doc_row[block_start:block_start + block_rows]
    own_places = places[block_start:block_start + block_rows]
    return (own_docs[:, None] == doc_row[None, key_low:key_high]) & (places[None, key_low:key_high] <= own_places[:, None])

def attend_block(query_rows, key_rows, value_rows, allowed, score_scale):
    scores = jnp.einsum('qkgd,skd->kgqs', as_wide(query_rows), as_wide(key_rows)) * score_scale
    scores = jnp.where(allowed[None, None], scores, -jnp.inf)
    row_max = lax.optimization_barrier(jnp.max(scores, axis=-1, keepdims=True))
    log_total = row_max + jnp.log(lax.optimization_barrier(jnp.sum(jnp.exp(scores - row_max), axis=-1, keepdims=True)))
    probabilities = jnp.exp(scores - log_total).astype(jnp.bfloat16)
    attn_out = jnp.einsum('kgqs,skd->qkgd', as_wide(probabilities), as_wide(value_rows))
    return (attn_out.astype(jnp.bfloat16), log_total)

def attend_back(query_rows, key_rows, value_rows, allowed, log_total, out_rows, grad_out, score_scale):
    query_wide = as_wide(query_rows)
    key_wide = as_wide(key_rows)
    value_wide = as_wide(value_rows)
    grad_wide = as_wide(grad_out)
    scores = jnp.einsum('qkgd,skd->kgqs', query_wide, key_wide) * score_scale
    scores = jnp.where(allowed[None, None], scores, -jnp.inf)
    probabilities = jnp.exp(scores - log_total)
    row_delta = jnp.einsum('qkgd,qkgd->kgq', grad_wide, as_wide(out_rows))
    grad_probs = jnp.einsum('qkgd,skd->kgqs', grad_wide, value_wide)
    grad_scores = (probabilities * (grad_probs - row_delta[..., None]) * score_scale).astype(jnp.bfloat16)
    scores_wide = as_wide(grad_scores)
    grad_query = jnp.einsum('kgqs,skd->qkgd', scores_wide, key_wide)
    grad_key = jnp.einsum('kgqs,qkgd->skd', scores_wide, query_wide)
    grad_value = jnp.einsum('kgqs,qkgd->skd', as_wide(probabilities.astype(jnp.bfloat16)), grad_wide)
    return (grad_query, grad_key, grad_value)

def shard_pass(shard_rows, doc_row, cotangent, weight_set):
    w_query, w_keyval, w_attn_out, w_gate_up, w_down, norm_gains = weight_set
    row_count = shard_rows.shape[0]
    group_size = HQ // KVH
    block_rows = min(512, row_count)
    score_scale = HD ** (-0.5)
    cosine, sine_table = rope_tables(doc_row, HD)
    block_starts = list(range(0, row_count, block_rows))
    windows = [(max(0, block_start - MAXLEN), block_start + block_rows) for block_start in block_starts]
    mask_list = [block_mask(doc_row, block_start, block_rows, windows[block_index][0], windows[block_index][1]) for block_index, block_start in enumerate(block_starts)]
    residual = shard_rows.astype(jnp.float32)
    stored = []
    for layer_index in range(LAYERS):
        gains = norm_gains[layer_index]
        inv_attn, normed = norm_apply(residual, gains[0])
        query_full = jnp.dot(normed, w_query[layer_index], preferred_element_type=jnp.float32).reshape(row_count, KVH, group_size, HD)
        keyval = jnp.dot(normed, w_keyval[layer_index].reshape(D, -1), preferred_element_type=jnp.float32).reshape(row_count, KVH, 2 * HD)
        query_rows = rotate(query_full, cosine, sine_table, 1.0).astype(jnp.bfloat16)
        key_rows = rotate(keyval[..., :HD], cosine, sine_table, 1.0).astype(jnp.bfloat16)
        value_rows = keyval[..., HD:].astype(jnp.bfloat16)
        out_list = []
        total_list = []
        for block_index, block_start in enumerate(block_starts):
            key_low, key_high = windows[block_index]
            out_block, log_total = attend_block(query_rows[block_start:block_start + block_rows], key_rows[key_low:key_high], value_rows[key_low:key_high], mask_list[block_index], score_scale)
            out_list.append(out_block)
            total_list.append(log_total)
        attended = jnp.concatenate(out_list, axis=0).reshape(row_count, HQ * HD)
        middle = residual + jnp.dot(attended, w_attn_out[layer_index], preferred_element_type=jnp.float32)
        inv_mlp, normed_mlp = norm_apply(middle, gains[1])
        gate_up = jnp.dot(normed_mlp, w_gate_up[layer_index].reshape(D, -1), preferred_element_type=jnp.float32).reshape(row_count, 2, FF)
        gate_value = gate_up[:, 0]
        up_value = gate_up[:, 1]
        hidden = (jax.nn.silu(gate_value) * up_value).astype(jnp.bfloat16)
        new_rows = middle + jnp.dot(hidden, w_down[layer_index], preferred_element_type=jnp.float32)
        stored.append((residual, inv_attn, normed, query_rows, key_rows, value_rows, attended, total_list, middle, inv_mlp, normed_mlp, gate_value, up_value, hidden))
        residual = new_rows
    output_rows = residual
    grad_rows = cotangent
    layer_grads = [None] * LAYERS
    for layer_index in reversed(range(LAYERS)):
        residual, inv_attn, normed, query_rows, key_rows, value_rows, attended, total_list, middle, inv_mlp, normed_mlp, gate_value, up_value, hidden = stored[layer_index]
        gains = norm_gains[layer_index]
        grad_bf = grad_rows.astype(jnp.bfloat16)
        grad_down = jnp.dot(hidden.T, grad_bf, preferred_element_type=jnp.float32)
        grad_hidden = jnp.dot(grad_bf, w_down[layer_index].T, preferred_element_type=jnp.float32)
        sigmoid_gate = jax.nn.sigmoid(gate_value)
        grad_gate = grad_hidden * up_value * sigmoid_gate * (1.0 + gate_value * (1.0 - sigmoid_gate))
        grad_up = grad_hidden * jax.nn.silu(gate_value)
        grad_gate_up = jnp.stack([grad_gate, grad_up], axis=1).astype(jnp.bfloat16).reshape(row_count, 2 * FF)
        grad_wgu = jnp.dot(normed_mlp.T, grad_gate_up, preferred_element_type=jnp.float32).reshape(D, 2, FF)
        grad_normed = jnp.dot(grad_gate_up, w_gate_up[layer_index].reshape(D, -1).T, preferred_element_type=jnp.float32)
        norm_part, grad_gain_mlp = norm_back(middle, inv_mlp, gains[1], grad_normed)
        grad_middle = grad_rows + norm_part
        middle_bf = grad_middle.astype(jnp.bfloat16)
        grad_wo = jnp.dot(attended.T, middle_bf, preferred_element_type=jnp.float32)
        grad_attended = jnp.dot(middle_bf, w_attn_out[layer_index].T, preferred_element_type=jnp.float32).astype(jnp.bfloat16).reshape(row_count, KVH, group_size, HD)
        attended_heads = attended.reshape(row_count, KVH, group_size, HD)
        grad_keys = jnp.zeros((row_count, KVH, HD), jnp.float32)
        grad_values = jnp.zeros((row_count, KVH, HD), jnp.float32)
        query_grads = []
        for block_index, block_start in enumerate(block_starts):
            block_stop = block_start + block_rows
            key_low, key_high = windows[block_index]
            grad_query_block, grad_key_part, grad_value_part = attend_back(query_rows[block_start:block_stop], key_rows[key_low:key_high], value_rows[key_low:key_high], mask_list[block_index], total_list[block_index], attended_heads[block_start:block_stop], grad_attended[block_start:block_stop], score_scale)
            query_grads.append(grad_query_block)
            pad_width = ((key_low, row_count - key_high), (0, 0), (0, 0))
            grad_keys = grad_keys + jnp.pad(grad_key_part, pad_width)
            grad_values = grad_values + jnp.pad(grad_value_part, pad_width)
        grad_query = rotate(jnp.concatenate(query_grads, axis=0), cosine, sine_table, -1.0).astype(jnp.bfloat16).reshape(row_count, HQ * HD)
        grad_keyval = jnp.concatenate([rotate(grad_keys, cosine, sine_table, -1.0), grad_values], axis=-1).astype(jnp.bfloat16).reshape(row_count, KVH * 2 * HD)
        grad_wq = jnp.dot(normed.T, grad_query, preferred_element_type=jnp.float32)
        grad_wkv = jnp.dot(normed.T, grad_keyval, preferred_element_type=jnp.float32).reshape(D, KVH, 2 * HD)
        grad_normed = jnp.dot(grad_query, w_query[layer_index].T, preferred_element_type=jnp.float32) + jnp.dot(grad_keyval, w_keyval[layer_index].reshape(D, -1).T, preferred_element_type=jnp.float32)
        norm_part, grad_gain_attn = norm_back(residual, inv_attn, gains[0], grad_normed)
        grad_rows = grad_middle + norm_part
        layer_grads[layer_index] = (grad_wq, grad_wkv, grad_wo, grad_wgu, grad_down, jnp.stack([grad_gain_attn, grad_gain_mlp]))
    stacked = tuple((jnp.stack([layer_grads[layer_index][member] for layer_index in range(LAYERS)]) for member in range(6)))
    return (output_rows, grad_rows, stacked)

def reference(block_input, doc_ids, w_query, w_keyval, w_attn_out, w_gate_up, w_down, norm_gains, out_cotangent):
    inputs = block_input.reshape(SHARDS, TOK_FS, D)
    cotangents = out_cotangent.reshape(SHARDS, TOK_FS, D)
    weight_set = (w_query, w_keyval, w_attn_out, w_gate_up, w_down, norm_gains)
    zero_grads = tuple((jnp.zeros(weight_array.shape, jnp.float32) for weight_array in weight_set))

    def one_shard(totals, shard_item):
        shard_rows, doc_row, cotangent = shard_item
        output_rows, grad_rows, shard_grads = shard_pass(shard_rows, doc_row, cotangent, weight_set)
        return (tuple((left_sum + right_sum for left_sum, right_sum in zip(totals, shard_grads))), (output_rows, grad_rows))
    totals, (outputs, grad_inputs) = lax.scan(one_shard, zero_grads, (inputs, doc_ids, cotangents))
    return (outputs.reshape(TOKENS, D), grad_inputs.reshape(TOKENS, D), totals[0], totals[1], totals[2], totals[3], totals[4], totals[5])
```

```python
import jax
import jax.numpy as jnp
from jax import lax
from jax.sharding import PartitionSpec as P

MAXLEN = 512


NORM_EPSILON = 1e-05
ROPE_BASE = 500000.0


def norm_apply(residual, gain):
    inverse = lax.rsqrt(jnp.mean(residual * residual, axis=-1, keepdims=True) + NORM_EPSILON)
    return (inverse, (residual * inverse * gain.astype(jnp.float32)).astype(jnp.bfloat16))


def norm_back(residual, inverse, gain, grad_normed):
    scaled = grad_normed * gain.astype(jnp.float32)
    grad_gain = jnp.sum(grad_normed * residual * inverse, axis=0)
    grad_residual = inverse * scaled - residual * inverse * inverse * inverse * jnp.mean(
        scaled * residual, axis=-1, keepdims=True
    )
    return (grad_residual, grad_gain)


def rope_tables(doc_row, head_size):
    places = jnp.arange(doc_row.shape[0], dtype=jnp.int32)
    doc_start = jnp.concatenate([jnp.array([True]), doc_row[1:] != doc_row[:-1]])
    starts = lax.cummax(jnp.where(doc_start, places, 0), axis=0)
    exponent = jnp.arange(head_size // 2, dtype=jnp.float32) * (-2.0 / head_size)
    angles = (places - starts).astype(jnp.float32)[:, None] * jnp.power(ROPE_BASE, exponent)[
        None, :
    ]
    return (jnp.cos(angles), jnp.sin(angles))


def rotate(vectors, cosine, sine_table, direction_sign):
    half_size = vectors.shape[-1] // 2
    table_shape = (vectors.shape[0],) + (1,) * (vectors.ndim - 2) + (half_size,)
    cos_part = cosine.reshape(table_shape)
    sin_part = direction_sign * sine_table.reshape(table_shape)
    first_half = vectors[..., :half_size]
    second = vectors[..., half_size:]
    return jnp.concatenate(
        [first_half * cos_part - second * sin_part, second * cos_part + first_half * sin_part],
        axis=-1,
    )


def block_mask(doc_row, block_start, block_rows, key_low, key_high):
    places = jnp.arange(doc_row.shape[0], dtype=jnp.int32)
    own_docs = doc_row[block_start : block_start + block_rows]
    own_places = places[block_start : block_start + block_rows]
    return (own_docs[:, None] == doc_row[None, key_low:key_high]) & (
        places[None, key_low:key_high] <= own_places[:, None]
    )


def attend_block(query_rows, key_rows, value_rows, allowed, score_scale):
    scores = (
        jnp.einsum("qkgd,skd->kgqs", query_rows, key_rows, preferred_element_type=jnp.float32)
        * score_scale
    )
    scores = jnp.where(allowed[None, None], scores, -jnp.inf)
    row_max = jnp.max(scores, axis=-1, keepdims=True)
    log_total = row_max + jnp.log(jnp.sum(jnp.exp(scores - row_max), axis=-1, keepdims=True))
    probabilities = jnp.exp(scores - log_total).astype(jnp.bfloat16)
    attn_out = jnp.einsum(
        "kgqs,skd->qkgd", probabilities, value_rows, preferred_element_type=jnp.float32
    )
    return (attn_out.astype(jnp.bfloat16), log_total)


def attend_back(
    query_rows, key_rows, value_rows, allowed, log_total, out_rows, grad_out, score_scale
):
    scores = (
        jnp.einsum("qkgd,skd->kgqs", query_rows, key_rows, preferred_element_type=jnp.float32)
        * score_scale
    )
    scores = jnp.where(allowed[None, None], scores, -jnp.inf)
    probabilities = jnp.exp(scores - log_total)
    row_delta = jnp.einsum("qkgd,qkgd->kgq", grad_out, out_rows, preferred_element_type=jnp.float32)
    grad_probs = jnp.einsum(
        "qkgd,skd->kgqs", grad_out, value_rows, preferred_element_type=jnp.float32
    )
    grad_scores = (probabilities * (grad_probs - row_delta[..., None]) * score_scale).astype(
        jnp.bfloat16
    )
    grad_query = jnp.einsum(
        "kgqs,skd->qkgd", grad_scores, key_rows, preferred_element_type=jnp.float32
    )
    grad_key = jnp.einsum(
        "kgqs,qkgd->skd", grad_scores, query_rows, preferred_element_type=jnp.float32
    )
    grad_value = jnp.einsum(
        "kgqs,qkgd->skd",
        probabilities.astype(jnp.bfloat16),
        grad_out,
        preferred_element_type=jnp.float32,
    )
    return (grad_query, grad_key, grad_value)


def per_device(
    block_input,
    doc_ids,
    w_query,
    w_keyval,
    w_attn_out,
    w_gate_up,
    w_down,
    norm_gains,
    out_cotangent,
):
    layers = w_query.shape[0]
    doc_row = doc_ids[0]
    row_count = doc_row.shape[0]
    local_rows = block_input.shape[0]
    kv_local = w_keyval.shape[2]
    head_size = w_keyval.shape[3] // 2
    group_size = w_query.shape[2] // (kv_local * head_size)
    block_rows = min(512, row_count)
    score_scale = head_size ** (-0.5)
    cosine, sine_table = rope_tables(doc_row, head_size)
    block_starts = list(range(0, row_count, block_rows))
    windows = [
        (max(0, block_start - MAXLEN), block_start + block_rows) for block_start in block_starts
    ]
    mask_list = [
        block_mask(
            doc_row, block_start, block_rows, windows[block_index][0], windows[block_index][1]
        )
        for block_index, block_start in enumerate(block_starts)
    ]

    def spread(rows_local):
        return lax.all_gather(rows_local, "tensor", axis=0, tiled=True)

    def collect(term_fn):
        return lax.psum_scatter(
            term_fn(jnp.int32(0), lax.axis_size("tensor") * local_rows).astype(jnp.bfloat16),
            "tensor",
            scatter_dimension=0,
            tiled=True,
        ).astype(jnp.float32)

    def spread_grad(rows_local):
        return lax.all_gather(rows_local, "tensor", axis=0, tiled=True)

    def collect_grad(term_fn):
        return lax.psum_scatter(
            term_fn(jnp.int32(0), lax.axis_size("tensor") * local_rows).astype(jnp.bfloat16),
            "tensor",
            scatter_dimension=0,
            tiled=True,
        ).astype(jnp.float32)

    residual = block_input.astype(jnp.float32)
    layer_index = 0
    weights = (
        lax.all_gather(w_query[layer_index], "fsdp", axis=0, tiled=True),
        lax.all_gather(w_keyval[layer_index], "fsdp", axis=0, tiled=True),
        lax.all_gather(w_attn_out[layer_index], "fsdp", axis=1, tiled=True),
        lax.all_gather(w_gate_up[layer_index], "fsdp", axis=0, tiled=True),
        lax.all_gather(w_down[layer_index], "fsdp", axis=1, tiled=True),
        lax.all_gather(norm_gains[layer_index], "fsdp", axis=1, tiled=True),
    )
    w_query_all, w_keyval_all, w_out_all, w_gate_all, w_down_all, gains_all = weights
    model_width = w_query_all.shape[0]
    inv_attn, normed = norm_apply(residual, gains_all[0])
    normed_all = spread(normed)
    query_full = jnp.dot(normed_all, w_query_all, preferred_element_type=jnp.float32).reshape(
        row_count, kv_local, group_size, head_size
    )
    keyval = jnp.dot(
        normed_all, w_keyval_all.reshape(model_width, -1), preferred_element_type=jnp.float32
    ).reshape(row_count, kv_local, 2 * head_size)
    query_rows = rotate(query_full, cosine, sine_table, 1.0).astype(jnp.bfloat16)
    key_rows = rotate(keyval[..., :head_size], cosine, sine_table, 1.0).astype(jnp.bfloat16)
    value_rows = keyval[..., head_size:].astype(jnp.bfloat16)
    out_list = []
    total_list = []
    for block_index, block_start in enumerate(block_starts):
        key_low, key_high = windows[block_index]
        out_block, log_total = attend_block(
            query_rows[block_start : block_start + block_rows],
            key_rows[key_low:key_high],
            value_rows[key_low:key_high],
            mask_list[block_index],
            score_scale,
        )
        out_list.append(out_block)
        total_list.append(log_total)
    attended = jnp.concatenate(out_list, axis=0).reshape(row_count, -1)

    def attn_term(row_start, row_size):
        return jnp.dot(attended, w_out_all, preferred_element_type=jnp.float32)

    middle = residual + collect(attn_term)
    inv_mlp, normed_mlp = norm_apply(middle, gains_all[1])
    normed_mlp_all = spread(normed_mlp)
    gate_up = jnp.dot(
        normed_mlp_all, w_gate_all.reshape(model_width, -1), preferred_element_type=jnp.float32
    ).reshape(row_count, 2, -1)
    gate_value = gate_up[:, 0]
    up_value = gate_up[:, 1]
    hidden = (jax.nn.silu(gate_value) * up_value).astype(jnp.bfloat16)

    def mlp_term(row_start, row_size):
        return jnp.dot(hidden, w_down_all, preferred_element_type=jnp.float32)

    new_rows = middle + collect(mlp_term)
    stored = [
        (
            residual,
            inv_attn,
            normed_all,
            query_rows,
            key_rows,
            value_rows,
            attended,
            total_list,
            middle,
            inv_mlp,
            normed_mlp_all,
            gate_value,
            up_value,
            hidden,
        )
    ]
    kept_weights = [weights]
    residual = new_rows
    output_rows = residual
    grad_rows = out_cotangent
    layer_grads = [None] * layers
    for layer_index in reversed(range(layers)):
        weights = kept_weights[layer_index]
        w_query_all, w_keyval_all, w_out_all, w_gate_all, w_down_all, gains_all = weights
        model_width = w_query_all.shape[0]
        (
            residual,
            inv_attn,
            normed_all,
            query_rows,
            key_rows,
            value_rows,
            attended,
            total_list,
            middle,
            inv_mlp,
            normed_mlp_all,
            gate_value,
            up_value,
            hidden,
        ) = stored[layer_index]
        grad_all = spread_grad(grad_rows.astype(jnp.bfloat16))
        grad_down = jnp.dot(hidden.T, grad_all, preferred_element_type=jnp.float32)
        grad_hidden = jnp.dot(grad_all, w_down_all.T, preferred_element_type=jnp.float32)
        sigmoid_gate = jax.nn.sigmoid(gate_value)
        grad_gate = (
            grad_hidden * up_value * sigmoid_gate * (1.0 + gate_value * (1.0 - sigmoid_gate))
        )
        grad_up = grad_hidden * jax.nn.silu(gate_value)
        grad_gate_up = (
            jnp.stack([grad_gate, grad_up], axis=1).astype(jnp.bfloat16).reshape(row_count, -1)
        )
        grad_wgu = jnp.dot(
            normed_mlp_all.T, grad_gate_up, preferred_element_type=jnp.float32
        ).reshape(w_gate_all.shape)

        def mlp_back(row_start, row_size):
            return jnp.dot(
                grad_gate_up,
                w_gate_all.reshape(model_width, -1).T,
                preferred_element_type=jnp.float32,
            )

        norm_part, grad_gain_mlp = norm_back(middle, inv_mlp, gains_all[1], collect_grad(mlp_back))
        grad_middle = grad_rows + norm_part
        middle_all = spread_grad(grad_middle.astype(jnp.bfloat16))
        grad_wo = jnp.dot(attended.T, middle_all, preferred_element_type=jnp.float32)
        grad_attended = (
            jnp.dot(middle_all, w_out_all.T, preferred_element_type=jnp.float32)
            .astype(jnp.bfloat16)
            .reshape(row_count, kv_local, group_size, head_size)
        )
        attended_heads = attended.reshape(row_count, kv_local, group_size, head_size)
        grad_keys = jnp.zeros((row_count, kv_local, head_size), jnp.float32)
        grad_values = jnp.zeros((row_count, kv_local, head_size), jnp.float32)
        query_grads = []
        for block_index, block_start in enumerate(block_starts):
            block_stop = block_start + block_rows
            key_low, key_high = windows[block_index]
            grad_query_block, grad_key_part, grad_value_part = attend_back(
                query_rows[block_start:block_stop],
                key_rows[key_low:key_high],
                value_rows[key_low:key_high],
                mask_list[block_index],
                total_list[block_index],
                attended_heads[block_start:block_stop],
                grad_attended[block_start:block_stop],
                score_scale,
            )
            query_grads.append(grad_query_block)
            pad_width = ((key_low, row_count - key_high), (0, 0), (0, 0))
            grad_keys = grad_keys + jnp.pad(grad_key_part, pad_width)
            grad_values = grad_values + jnp.pad(grad_value_part, pad_width)
        grad_query = (
            rotate(jnp.concatenate(query_grads, axis=0), cosine, sine_table, -1.0)
            .astype(jnp.bfloat16)
            .reshape(row_count, -1)
        )
        grad_keyval = (
            jnp.concatenate([rotate(grad_keys, cosine, sine_table, -1.0), grad_values], axis=-1)
            .astype(jnp.bfloat16)
            .reshape(row_count, -1)
        )
        grad_wq = jnp.dot(normed_all.T, grad_query, preferred_element_type=jnp.float32)
        grad_wkv = jnp.dot(normed_all.T, grad_keyval, preferred_element_type=jnp.float32).reshape(
            w_keyval_all.shape
        )

        def attn_back(row_start, row_size):
            return jnp.dot(grad_query, w_query_all.T, preferred_element_type=jnp.float32) + jnp.dot(
                grad_keyval,
                w_keyval_all.reshape(model_width, -1).T,
                preferred_element_type=jnp.float32,
            )

        norm_part, grad_gain_attn = norm_back(
            residual, inv_attn, gains_all[0], collect_grad(attn_back)
        )
        grad_rows = grad_middle + norm_part
        gain_total = lax.psum(jnp.stack([grad_gain_attn, grad_gain_mlp]), "tensor")
        local_set = (grad_wq, grad_wkv, grad_wo, grad_wgu, grad_down, gain_total)
        layer_grads[layer_index] = (
            lax.psum_scatter(local_set[0].astype(jnp.bfloat16), "fsdp", scatter_dimension=0, tiled=True).astype(jnp.float32),
            lax.psum_scatter(local_set[1].astype(jnp.bfloat16), "fsdp", scatter_dimension=0, tiled=True).astype(jnp.float32),
            lax.psum_scatter(local_set[2].astype(jnp.bfloat16), "fsdp", scatter_dimension=1, tiled=True).astype(jnp.float32),
            lax.psum_scatter(local_set[3].astype(jnp.bfloat16), "fsdp", scatter_dimension=0, tiled=True).astype(jnp.float32),
            lax.psum_scatter(local_set[4].astype(jnp.bfloat16), "fsdp", scatter_dimension=1, tiled=True).astype(jnp.float32),
            lax.psum_scatter(local_set[5], "fsdp", scatter_dimension=1, tiled=True),
        )
    stacked = tuple((jnp.stack([layer_grads[0][member]]) for member in range(6)))
    return (
        output_rows,
        grad_rows,
        stacked[0],
        stacked[1],
        stacked[2],
        stacked[3],
        stacked[4],
        stacked[5],
    )


def solution(mesh):
    return jax.shard_map(
        per_device,
        mesh=mesh,
        in_specs=(
            P(("fsdp", "tensor"), None),
            P("fsdp", None),
            P(None, "fsdp", "tensor"),
            P(None, "fsdp", "tensor", None),
            P(None, "tensor", "fsdp"),
            P(None, "fsdp", None, "tensor"),
            P(None, "tensor", "fsdp"),
            P(None, None, "fsdp"),
            P(("fsdp", "tensor"), None),
        ),
        out_specs=(
            P(("fsdp", "tensor"), None),
            P(("fsdp", "tensor"), None),
            P(None, "fsdp", "tensor"),
            P(None, "fsdp", "tensor", None),
            P(None, "tensor", "fsdp"),
            P(None, "fsdp", None, "tensor"),
            P(None, "tensor", "fsdp"),
            P(None, None, "fsdp"),
        ),
        check_vma=False,
    )
```

```python
import jax
import jax.numpy as jnp
from jax import lax
from jax.sharding import PartitionSpec as P


MAXLEN = 512


NORM_EPSILON = 1e-05
ROPE_BASE = 500000.0


def norm_apply(residual, gain):
    inverse = lax.rsqrt(jnp.mean(residual * residual, axis=-1, keepdims=True) + NORM_EPSILON)
    return (inverse, (residual * inverse * gain.astype(jnp.float32)).astype(jnp.bfloat16))


def norm_back(residual, inverse, gain, grad_normed):
    scaled = grad_normed * gain.astype(jnp.float32)
    grad_gain = jnp.sum(grad_normed * residual * inverse, axis=0)
    grad_residual = inverse * scaled - residual * inverse * inverse * inverse * jnp.mean(
        scaled * residual, axis=-1, keepdims=True
    )
    return (grad_residual, grad_gain)


def rope_tables(doc_row, head_size):
    places = jnp.arange(doc_row.shape[0], dtype=jnp.int32)
    doc_start = jnp.concatenate([jnp.array([True]), doc_row[1:] != doc_row[:-1]])
    starts = lax.cummax(jnp.where(doc_start, places, 0), axis=0)
    exponent = jnp.arange(head_size // 2, dtype=jnp.float32) * (-2.0 / head_size)
    angles = (places - starts).astype(jnp.float32)[:, None] * jnp.power(ROPE_BASE, exponent)[
        None, :
    ]
    return (jnp.cos(angles), jnp.sin(angles))


def rotate(vectors, cosine, sine_table, direction_sign):
    half_size = vectors.shape[-1] // 2
    table_shape = (vectors.shape[0],) + (1,) * (vectors.ndim - 2) + (half_size,)
    cos_part = cosine.reshape(table_shape)
    sin_part = direction_sign * sine_table.reshape(table_shape)
    first_half = vectors[..., :half_size]
    second = vectors[..., half_size:]
    return jnp.concatenate(
        [first_half * cos_part - second * sin_part, second * cos_part + first_half * sin_part],
        axis=-1,
    )


def block_mask(doc_row, block_start, block_rows, key_low, key_high):
    places = jnp.arange(doc_row.shape[0], dtype=jnp.int32)
    own_docs = doc_row[block_start : block_start + block_rows]
    own_places = places[block_start : block_start + block_rows]
    return (own_docs[:, None] == doc_row[None, key_low:key_high]) & (
        places[None, key_low:key_high] <= own_places[:, None]
    )


def attend_block(query_rows, key_rows, value_rows, allowed, score_scale):
    scores = (
        jnp.einsum("qkgd,skd->kgqs", query_rows, key_rows, preferred_element_type=jnp.float32)
        * score_scale
    )
    scores = jnp.where(allowed[None, None], scores, -jnp.inf)
    row_max = jnp.max(scores, axis=-1, keepdims=True)
    log_total = row_max + jnp.log(jnp.sum(jnp.exp(scores - row_max), axis=-1, keepdims=True))
    probabilities = jnp.exp(scores - log_total).astype(jnp.bfloat16)
    attn_out = jnp.einsum(
        "kgqs,skd->qkgd", probabilities, value_rows, preferred_element_type=jnp.float32
    )
    return (attn_out.astype(jnp.bfloat16), log_total)


def attend_back(
    query_rows, key_rows, value_rows, allowed, log_total, out_rows, grad_out, score_scale
):
    scores = (
        jnp.einsum("qkgd,skd->kgqs", query_rows, key_rows, preferred_element_type=jnp.float32)
        * score_scale
    )
    scores = jnp.where(allowed[None, None], scores, -jnp.inf)
    probabilities = jnp.exp(scores - log_total)
    row_delta = jnp.einsum("qkgd,qkgd->kgq", grad_out, out_rows, preferred_element_type=jnp.float32)
    grad_probs = jnp.einsum(
        "qkgd,skd->kgqs", grad_out, value_rows, preferred_element_type=jnp.float32
    )
    grad_scores = (probabilities * (grad_probs - row_delta[..., None]) * score_scale).astype(
        jnp.bfloat16
    )
    grad_query = jnp.einsum(
        "kgqs,skd->qkgd", grad_scores, key_rows, preferred_element_type=jnp.float32
    )
    grad_key = jnp.einsum(
        "kgqs,qkgd->skd", grad_scores, query_rows, preferred_element_type=jnp.float32
    )
    grad_value = jnp.einsum(
        "kgqs,qkgd->skd",
        probabilities.astype(jnp.bfloat16),
        grad_out,
        preferred_element_type=jnp.float32,
    )
    return (grad_query, grad_key, grad_value)


def per_device(
    block_input,
    doc_ids,
    w_query,
    w_keyval,
    w_attn_out,
    w_gate_up,
    w_down,
    norm_gains,
    out_cotangent,
):
    f32, bf16 = jnp.float32, jnp.bfloat16
    ring = lax.axis_size("tensor")
    place = lax.axis_index("tensor")
    ring_pairs = [(i, (i + 1) % ring) for i in range(ring)]
    doc_row = doc_ids[0]
    row_count = doc_row.shape[0]
    local_rows, _ = block_input.shape
    kv_local = w_keyval.shape[2]
    head_size = w_keyval.shape[3] // 2
    query_width = w_query.shape[2]
    group_size = query_width // (kv_local * head_size)
    block_rows = min(512, row_count)
    score_scale = head_size ** (-0.5)

    def dot(a, b):
        return jnp.dot(a, b, preferred_element_type=f32)

    def dot_nt(a, b):
        return lax.dot_general(a, b, (((1,), (1,)), ((), ())), preferred_element_type=f32)

    def dot_tn(a, b):
        return lax.dot_general(a, b, (((0,), (0,)), ((), ())), preferred_element_type=f32)

    def shift(rows):
        return lax.ppermute(rows, "tensor", ring_pairs)

    def after(value, gate):
        return lax.optimization_barrier((value, gate))[0]

    def block_start_of(step):
        return lax.rem(place - step + ring, ring) * local_rows

    def spread(rows):
        blocks = [rows]
        for _ in range(ring - 1):
            blocks.append(shift(blocks[-1]))
        return blocks

    def in_order(blocks):
        whole = jnp.zeros((ring * local_rows,) + blocks[0].shape[1:], blocks[0].dtype)
        for step, block in enumerate(blocks):
            whole = lax.dynamic_update_slice_in_dim(whole, block, block_start_of(step), 0)
        return whole

    def rows_of(whole, step):
        return lax.dynamic_slice_in_dim(whole, block_start_of(step), local_rows, 0)

    def scatter_sum(grad):
        return lax.psum_scatter(grad, "fsdp", scatter_dimension=0, tiled=True).astype(f32)

    def collect(parts, last_gate=None):
        total = parts[1 % ring].astype(f32)
        for step in range(2, ring + 1):
            if step == ring and last_gate is not None:
                total = after(total, last_gate)
            total = shift(total.astype(bf16)).astype(f32) + parts[step % ring]
        return total

    w_qkv_local = jnp.concatenate(
        [w_query[0], w_keyval[0].reshape(w_keyval.shape[1], -1)], axis=1
    )
    w_qkv = lax.all_gather(w_qkv_local, "fsdp", axis=0, tiled=True)
    gains_all = lax.all_gather(norm_gains[0], "fsdp", axis=1, tiled=True)
    w_out_all = lax.all_gather(w_attn_out[0], "fsdp", axis=1, tiled=True)
    w_gu_all = lax.all_gather(
        jnp.swapaxes(w_gate_up[0], 0, 1), "fsdp", axis=1, tiled=True
    )
    w_down_all = lax.all_gather(w_down[0], "fsdp", axis=1, tiled=True)
    w_gate, w_up = w_gu_all[0], w_gu_all[1]

    cosine, sine_table = rope_tables(doc_row, head_size)
    block_starts = list(range(0, row_count, block_rows))
    windows = [
        (max(0, start - MAXLEN), start + block_rows) for start in block_starts
    ]
    mask_list = [
        block_mask(doc_row, start, block_rows, windows[index][0], windows[index][1])
        for index, start in enumerate(block_starts)
    ]

    input_blocks = spread(block_input)
    grad_blocks = spread(after(out_cotangent.astype(bf16), input_blocks[-1]))
    normed_pairs = [norm_apply(block.astype(f32), gains_all[0]) for block in input_blocks]
    residual = block_input.astype(f32)
    inv_attn = normed_pairs[0][0]
    normed_all = in_order([pair[1] for pair in normed_pairs])
    qkv = dot(normed_all, w_qkv)
    query_rows = rotate(
        qkv[:, :query_width].reshape(row_count, kv_local, group_size, head_size),
        cosine, sine_table, 1.0,
    ).astype(bf16)
    keyval = qkv[:, query_width:].reshape(row_count, kv_local, 2 * head_size)
    key_rows = rotate(keyval[..., :head_size], cosine, sine_table, 1.0).astype(bf16)
    value_rows = keyval[..., head_size:].astype(bf16)
    out_list = []
    total_list = []
    for block_index, block_start in enumerate(block_starts):
        key_low, key_high = windows[block_index]
        attend_inputs = (
            query_rows[block_start : block_start + block_rows],
            key_rows[key_low:key_high],
            value_rows[key_low:key_high],
        )
        if block_index == len(block_starts) - 1:
            attend_inputs = after(attend_inputs, grad_blocks[1 % ring])
        out_block, log_total = attend_block(
            *attend_inputs,
            mask_list[block_index],
            score_scale,
        )
        out_list.append(out_block)
        total_list.append(log_total)
    attended = jnp.concatenate(out_list, axis=0).reshape(row_count, -1)
    attended = after(attended, grad_blocks[2 % ring])
    middle = residual + collect(
        [dot(rows_of(attended, step), w_out_all) for step in range(ring)]
    )
    inv_mlp, normed_mlp = norm_apply(middle, gains_all[1])

    normed_mlp_blocks = [normed_mlp]
    hidden_blocks, dgate_blocks, dup_blocks, back_parts = [], [], [], []
    for step in range(ring):
        if step == 1:
            normed_mlp_blocks.append(shift(normed_mlp))
        elif step > 1:
            gate = dup_blocks[0] if step == 2 else back_parts[step - 2]
            normed_mlp_blocks.append(shift(after(normed_mlp_blocks[-1], gate)))
        rows = normed_mlp_blocks[step]
        if step == 1:
            rows = after(rows, (dgate_blocks[0], dup_blocks[0]))
        elif step > 1:
            rows = after(rows, back_parts[step - 1])
        gate = dot(rows, w_gate)
        up = dot(rows, w_up)
        grad_hidden = dot_nt(grad_blocks[step], w_down_all)
        sigmoid_gate = jax.nn.sigmoid(gate)
        silu_gate = gate * sigmoid_gate
        hidden_blocks.append((silu_gate * up).astype(bf16))
        dgate = (grad_hidden * up * sigmoid_gate * (1.0 + gate * (1.0 - sigmoid_gate))).astype(bf16)
        dup = (grad_hidden * silu_gate).astype(bf16)
        dgate_blocks.append(dgate)
        dup_blocks.append(dup)
        back_parts.append(dot_nt(dgate, w_gate) + dot_nt(dup, w_up))
    grad_normed_mlp = collect(back_parts)
    grad_down = dot_tn(in_order(grad_blocks), in_order(hidden_blocks)).astype(bf16)
    normed_mlp_all = in_order(normed_mlp_blocks)
    grad_wgate = dot_tn(normed_mlp_all, in_order(dgate_blocks)).astype(bf16)
    grad_wup = dot_tn(normed_mlp_all, in_order(dup_blocks)).astype(bf16)
    grad_normed_mlp = after(grad_normed_mlp, (grad_down, grad_wgate))
    grad_down = jnp.swapaxes(scatter_sum(grad_down), 0, 1)
    grad_wgate = scatter_sum(grad_wgate)
    norm_part, grad_gain_mlp = norm_back(middle, inv_mlp, gains_all[1], grad_normed_mlp)
    grad_middle = out_cotangent + norm_part

    middle_blocks = spread(grad_middle.astype(bf16))
    do_parts = [dot_nt(block, w_out_all).astype(bf16) for block in middle_blocks]
    grad_attended = in_order(do_parts).reshape(row_count, kv_local, group_size, head_size)
    middle_all = in_order(middle_blocks)

    grad_attended = after(grad_attended, grad_wup)
    grad_wup = scatter_sum(grad_wup)
    grad_wgu = jnp.stack([grad_wgate, grad_wup], axis=1)
    grad_wo = jnp.swapaxes(scatter_sum(dot_tn(middle_all, attended).astype(bf16)), 0, 1)

    out_parts = [dot(hidden, w_down_all) for hidden in hidden_blocks]
    out_totals = [after(out_parts[1 % ring], middle_blocks[-1]).astype(bf16)]
    for step in range(2, ring + 1):
        out_totals.append((shift(out_totals[-1]).astype(f32) + out_parts[step % ring]))
        if step < ring:
            out_totals[-1] = out_totals[-1].astype(bf16)
    output_rows = middle + out_totals[-1]

    attended_heads = attended.reshape(row_count, kv_local, group_size, head_size)
    grad_keys = jnp.zeros((row_count, kv_local, head_size), f32)
    grad_values = jnp.zeros((row_count, kv_local, head_size), f32)
    query_grads = []
    for block_index, block_start in enumerate(block_starts):
        block_stop = block_start + block_rows
        key_low, key_high = windows[block_index]
        grad_out = after(grad_attended[block_start:block_stop], out_totals[block_index])
        grad_query_block, grad_key_part, grad_value_part = attend_back(
            query_rows[block_start:block_stop],
            key_rows[key_low:key_high],
            value_rows[key_low:key_high],
            mask_list[block_index],
            total_list[block_index],
            attended_heads[block_start:block_stop],
            grad_out,
            score_scale,
        )
        query_grads.append(grad_query_block)
        pad_width = ((key_low, row_count - key_high), (0, 0), (0, 0))
        grad_keys = grad_keys + jnp.pad(grad_key_part, pad_width)
        grad_values = grad_values + jnp.pad(grad_value_part, pad_width)
    grad_query = (
        rotate(jnp.concatenate(query_grads, axis=0), cosine, sine_table, -1.0)
        .astype(bf16)
        .reshape(row_count, -1)
    )
    grad_keyval = (
        jnp.concatenate([rotate(grad_keys, cosine, sine_table, -1.0), grad_values], axis=-1)
        .astype(bf16)
        .reshape(row_count, -1)
    )
    grad_qkv = jnp.concatenate([grad_query, grad_keyval], axis=1)
    grad_qkv = after(grad_qkv, out_totals[-2])
    in_parts = [dot_nt(rows_of(grad_qkv, step), w_qkv) for step in range(ring)]
    grad_normed = collect(in_parts, output_rows)
    norm_part, _ = norm_back(residual, inv_attn, gains_all[0], grad_normed)
    grad_rows = grad_middle + norm_part

    grad_gain_attn = sum(
        jnp.sum(part * block.astype(f32) * pair[0], axis=0)
        for part, block, pair in zip(in_parts, input_blocks, normed_pairs)
    )
    grad_wqkv = dot_tn(normed_all, grad_qkv).astype(bf16)
    gain_columns = jnp.stack([grad_gain_attn, grad_gain_mlp], axis=1).astype(bf16)
    gain_columns = jnp.pad(gain_columns, ((0, 0), (0, 126)))
    packed = scatter_sum(jnp.concatenate([grad_wqkv, gain_columns], axis=1))
    qkv_width = grad_wqkv.shape[1]
    grad_wq = packed[:, :query_width]
    grad_wkv = packed[:, query_width:qkv_width].reshape(-1, kv_local, 2 * head_size)
    gain_part = packed[:, qkv_width : qkv_width + 2]
    gain_total = gain_part
    for _ in range(ring - 1):
        gain_part = shift(gain_part)
        gain_total = gain_total + gain_part
    return (
        output_rows,
        grad_rows,
        grad_wq[None],
        grad_wkv[None],
        grad_wo[None],
        grad_wgu[None],
        grad_down[None],
        gain_total.T[None],
    )


def solution(mesh):
    return jax.shard_map(
        per_device,
        mesh=mesh,
        in_specs=(
            P(("fsdp", "tensor"), None),
            P("fsdp", None),
            P(None, "fsdp", "tensor"),
            P(None, "fsdp", "tensor", None),
            P(None, "tensor", "fsdp"),
            P(None, "fsdp", None, "tensor"),
            P(None, "tensor", "fsdp"),
            P(None, None, "fsdp"),
            P(("fsdp", "tensor"), None),
        ),
        out_specs=(
            P(("fsdp", "tensor"), None),
            P(("fsdp", "tensor"), None),
            P(None, "fsdp", "tensor"),
            P(None, "fsdp", "tensor", None),
            P(None, "tensor", "fsdp"),
            P(None, "fsdp", None, "tensor"),
            P(None, "tensor", "fsdp"),
            P(None, None, "fsdp"),
        ),
        check_vma=False,
    )
```

```python
import functools

import jax
import jax.numpy as jnp
from jax import lax
from jax.experimental import pallas as pl
from jax.experimental.pallas import tpu as pltpu
from jax.sharding import PartitionSpec as P


MAXLEN = 512


NORM_EPSILON = 1e-05
ROPE_BASE = 500000.0


def norm_apply(residual, gain):
    inverse = lax.rsqrt(jnp.mean(residual * residual, axis=-1, keepdims=True) + NORM_EPSILON)
    return (inverse, (residual * inverse * gain.astype(jnp.float32)).astype(jnp.bfloat16))


def norm_back(residual, inverse, gain, grad_normed):
    scaled = grad_normed * gain.astype(jnp.float32)
    grad_gain = jnp.sum(grad_normed * residual * inverse, axis=0)
    grad_residual = inverse * scaled - residual * inverse * inverse * inverse * jnp.mean(
        scaled * residual, axis=-1, keepdims=True
    )
    return (grad_residual, grad_gain)


def rope_tables(doc_row, head_size):
    places = jnp.arange(doc_row.shape[0], dtype=jnp.int32)
    doc_start = jnp.concatenate([jnp.array([True]), doc_row[1:] != doc_row[:-1]])
    starts = lax.cummax(jnp.where(doc_start, places, 0), axis=0)
    exponent = jnp.arange(head_size // 2, dtype=jnp.float32) * (-2.0 / head_size)
    angles = (places - starts).astype(jnp.float32)[:, None] * jnp.power(ROPE_BASE, exponent)[
        None, :
    ]
    return (jnp.cos(angles), jnp.sin(angles))


def rotate(vectors, cosine, sine_table, direction_sign):
    half_size = vectors.shape[-1] // 2
    table_shape = (vectors.shape[0],) + (1,) * (vectors.ndim - 2) + (half_size,)
    cos_part = cosine.reshape(table_shape)
    sin_part = direction_sign * sine_table.reshape(table_shape)
    first_half = vectors[..., :half_size]
    second = vectors[..., half_size:]
    return jnp.concatenate(
        [first_half * cos_part - second * sin_part, second * cos_part + first_half * sin_part],
        axis=-1,
    )


def block_mask(doc_row, block_start, block_rows, key_low, key_high):
    places = jnp.arange(doc_row.shape[0], dtype=jnp.int32)
    own_docs = doc_row[block_start : block_start + block_rows]
    own_places = places[block_start : block_start + block_rows]
    return (own_docs[:, None] == doc_row[None, key_low:key_high]) & (
        places[None, key_low:key_high] <= own_places[:, None]
    )


def attend_block(query_rows, key_rows, value_rows, allowed, score_scale):
    scores = (
        jnp.einsum("qkgd,skd->kgqs", query_rows, key_rows, preferred_element_type=jnp.float32)
        * score_scale
    )
    scores = jnp.where(allowed[None, None], scores, -jnp.inf)
    row_max = jnp.max(scores, axis=-1, keepdims=True)
    log_total = row_max + jnp.log(jnp.sum(jnp.exp(scores - row_max), axis=-1, keepdims=True))
    probabilities = jnp.exp(scores - log_total).astype(jnp.bfloat16)
    attn_out = jnp.einsum(
        "kgqs,skd->qkgd", probabilities, value_rows, preferred_element_type=jnp.float32
    )
    return (attn_out.astype(jnp.bfloat16), log_total)


def attend_back(
    query_rows, key_rows, value_rows, allowed, log_total, out_rows, grad_out, score_scale
):
    scores = (
        jnp.einsum("qkgd,skd->kgqs", query_rows, key_rows, preferred_element_type=jnp.float32)
        * score_scale
    )
    scores = jnp.where(allowed[None, None], scores, -jnp.inf)
    probabilities = jnp.exp(scores - log_total)
    row_delta = jnp.einsum("qkgd,qkgd->kgq", grad_out, out_rows, preferred_element_type=jnp.float32)
    grad_probs = jnp.einsum(
        "qkgd,skd->kgqs", grad_out, value_rows, preferred_element_type=jnp.float32
    )
    grad_scores = (probabilities * (grad_probs - row_delta[..., None]) * score_scale).astype(
        jnp.bfloat16
    )
    grad_query = jnp.einsum(
        "kgqs,skd->qkgd", grad_scores, key_rows, preferred_element_type=jnp.float32
    )
    grad_key = jnp.einsum(
        "kgqs,qkgd->skd", grad_scores, query_rows, preferred_element_type=jnp.float32
    )
    grad_value = jnp.einsum(
        "kgqs,qkgd->skd",
        probabilities.astype(jnp.bfloat16),
        grad_out,
        preferred_element_type=jnp.float32,
    )
    return (grad_query, grad_key, grad_value)


def mlp_kernel(reused, *refs):
    x_ref, g_ref, w_gu_ref, w_down_ref = refs[:4]
    hidden_ref, dgate_ref, dup_ref, x_all_ref, g_all_ref, back_ref, out_ref = refs[4 + reused :]
    first = pl.program_id(0) == 0
    dims = (((1,), (1,)), ((), ()))
    x = x_ref[...]
    g = g_ref[...]
    w_gate = w_gu_ref[0]
    w_up = w_gu_ref[1]
    w_down = w_down_ref[...]
    gate = jnp.dot(x, w_gate, preferred_element_type=jnp.float32)
    up = jnp.dot(x, w_up, preferred_element_type=jnp.float32)
    grad_hidden = lax.dot_general(g, w_down, dims, preferred_element_type=jnp.float32)
    sigmoid_gate = 1.0 / (1.0 + jnp.exp(-gate))
    silu_gate = gate * sigmoid_gate
    hidden = (silu_gate * up).astype(jnp.bfloat16)
    dgate = (grad_hidden * up * sigmoid_gate * (1.0 + gate * (1.0 - sigmoid_gate))).astype(
        jnp.bfloat16
    )
    dup = (grad_hidden * silu_gate).astype(jnp.bfloat16)
    hidden_ref[...] = hidden
    dgate_ref[...] = dgate
    dup_ref[...] = dup

    @pl.when(first)
    def _():
        x_all_ref[...] = x
        g_all_ref[...] = g
        out_ref[...] = jnp.zeros_like(out_ref)
        back_ref[...] = jnp.zeros_like(back_ref)

    out_ref[...] += jnp.dot(hidden, w_down, preferred_element_type=jnp.float32)
    back_ref[...] += lax.dot_general(
        dgate, w_gate, dims, preferred_element_type=jnp.float32
    ) + lax.dot_general(dup, w_up, dims, preferred_element_type=jnp.float32)


def mlp_block(step, ring, x, g, w_gu, w_down, kept):
    rows, width = x.shape
    hidden_width = w_down.shape[0]
    tile = min(512, hidden_width)
    bf16, f32 = jnp.bfloat16, jnp.float32
    wide = jax.ShapeDtypeStruct((ring * rows, hidden_width), bf16)
    whole = jax.ShapeDtypeStruct((ring * rows, width), bf16)
    part = jax.ShapeDtypeStruct((rows, width), f32)
    wide_spec = pl.BlockSpec((rows, tile), lambda t: (step, t))
    whole_spec = pl.BlockSpec((rows, width), lambda t: (step, 0))
    block_spec = pl.BlockSpec((rows, width), lambda t: (0, 0))
    reused = len(kept)
    return pl.pallas_call(
        functools.partial(mlp_kernel, reused),
        grid=(hidden_width // tile,),
        out_shape=(wide, wide, wide, whole, whole, part, part),
        in_specs=[
            block_spec,
            block_spec,
            pl.BlockSpec((2, width, tile), lambda t: (0, 0, t)),
            pl.BlockSpec((tile, width), lambda t: (t, 0)),
        ]
        + [pl.BlockSpec(memory_space=pl.ANY)] * reused,
        out_specs=(wide_spec, wide_spec, wide_spec, whole_spec, whole_spec, block_spec, block_spec),
        input_output_aliases={4 + i: i for i in range(reused)},
        cost_estimate=pl.CostEstimate(
            flops=12 * rows * width * hidden_width,
            bytes_accessed=6 * width * hidden_width + 12 * rows * width,
            transcendentals=rows * hidden_width,
        ),
        compiler_params=pltpu.CompilerParams(vmem_limit_bytes=44 << 20),
        name="mlp_block",
    )(x, g, w_gu, w_down, *kept)


def per_device(
    block_input,
    doc_ids,
    w_query,
    w_keyval,
    w_attn_out,
    w_gate_up,
    w_down,
    norm_gains,
    out_cotangent,
):
    f32, bf16 = jnp.float32, jnp.bfloat16
    ring = lax.axis_size("tensor")
    place = lax.axis_index("tensor")
    ring_pairs = [(i, (i + 1) % ring) for i in range(ring)]
    doc_row = doc_ids[0]
    row_count = doc_row.shape[0]
    local_rows, _ = block_input.shape
    kv_local = w_keyval.shape[2]
    head_size = w_keyval.shape[3] // 2
    query_width = w_query.shape[2]
    group_size = query_width // (kv_local * head_size)
    block_rows = min(512, row_count)
    score_scale = head_size ** (-0.5)

    def dot(a, b):
        return jnp.dot(a, b, preferred_element_type=f32)

    def dot_nt(a, b):
        return lax.dot_general(a, b, (((1,), (1,)), ((), ())), preferred_element_type=f32)

    def dot_tn(a, b):
        return lax.dot_general(a, b, (((0,), (0,)), ((), ())), preferred_element_type=f32)

    def shift(rows):
        return lax.ppermute(rows, "tensor", ring_pairs)

    def after(value, gate):
        return lax.optimization_barrier((value, gate))[0]

    def block_start_of(step):
        return lax.rem(place - step + ring, ring) * local_rows

    def spread(rows):
        blocks = [rows]
        for _ in range(1, ring):
            blocks.append(shift(blocks[-1]))
        return blocks

    def in_order(blocks):
        whole = jnp.zeros((ring * local_rows,) + blocks[0].shape[1:], blocks[0].dtype)
        for step, block in enumerate(blocks):
            whole = lax.dynamic_update_slice_in_dim(whole, block, block_start_of(step), 0)
        return whole

    def rows_of(whole, step):
        return lax.dynamic_slice_in_dim(whole, block_start_of(step), local_rows, 0)

    def collect(parts, last_gate=None):
        total = parts[1 % ring].astype(f32)
        for step in range(2, ring + 1):
            if step == ring and last_gate is not None:
                total = after(total, last_gate)
            total = shift(total.astype(bf16)).astype(f32) + parts[step % ring]
        return total

    w_qkv_local = jnp.concatenate(
        [w_query[0], w_keyval[0].reshape(w_keyval.shape[1], -1)], axis=1
    )
    w_qkv = lax.all_gather(w_qkv_local, "fsdp", axis=0, tiled=True)
    gains_all = lax.all_gather(norm_gains[0], "fsdp", axis=1, tiled=True)
    w_out_all = lax.all_gather(w_attn_out[0], "fsdp", axis=1, tiled=True)
    w_gu_all = lax.all_gather(
        jnp.swapaxes(w_gate_up[0], 0, 1), "fsdp", axis=1, tiled=True
    )
    w_down_all = lax.all_gather(w_down[0], "fsdp", axis=1, tiled=True)

    cosine, sine_table = rope_tables(doc_row, head_size)
    block_starts = list(range(0, row_count, block_rows))
    windows = [
        (max(0, start - MAXLEN), start + block_rows) for start in block_starts
    ]
    mask_list = [
        block_mask(doc_row, start, block_rows, windows[index][0], windows[index][1])
        for index, start in enumerate(block_starts)
    ]

    input_blocks = spread(block_input)
    grad_blocks = spread(after(out_cotangent.astype(bf16), input_blocks[-1]))
    normed_pairs = [norm_apply(block.astype(f32), gains_all[0]) for block in input_blocks]
    residual = block_input.astype(f32)
    inv_attn = normed_pairs[0][0]
    normed_all = in_order([pair[1] for pair in normed_pairs])
    qkv = dot(normed_all, w_qkv)
    query_rows = rotate(
        qkv[:, :query_width].reshape(row_count, kv_local, group_size, head_size),
        cosine, sine_table, 1.0,
    ).astype(bf16)
    keyval = qkv[:, query_width:].reshape(row_count, kv_local, 2 * head_size)
    key_rows = rotate(keyval[..., :head_size], cosine, sine_table, 1.0).astype(bf16)
    value_rows = keyval[..., head_size:].astype(bf16)
    out_list = []
    total_list = []
    for block_index, block_start in enumerate(block_starts):
        key_low, key_high = windows[block_index]
        attend_inputs = (
            query_rows[block_start : block_start + block_rows],
            key_rows[key_low:key_high],
            value_rows[key_low:key_high],
        )
        if block_index > 0:
            attend_inputs = after(attend_inputs, out_list[-1])
        out_block, log_total = attend_block(
            *attend_inputs,
            mask_list[block_index],
            score_scale,
        )
        out_list.append(out_block)
        total_list.append(log_total)
    attended = jnp.concatenate(out_list, axis=0).reshape(row_count, -1)
    middle = residual + collect([dot(rows_of(attended, step), w_out_all) for step in range(ring)])
    inv_mlp, normed_mlp = norm_apply(middle, gains_all[1])

    normed_mlp_blocks = [normed_mlp]
    kept, back_parts, out_parts = (), [], []
    for step in range(ring):
        if step > 0:
            source = normed_mlp_blocks[-1]
            if step > 1:
                source = after(source, back_parts[step - 2])
            normed_mlp_blocks.append(shift(source))
        rows = normed_mlp_blocks[step]
        if step > 0:
            rows = after(rows, back_parts[step - 1])
        *kept, back_part, out_part = mlp_block(
            step, ring, rows, grad_blocks[step], w_gu_all, w_down_all, tuple(kept)
        )
        back_parts.append(back_part)
        out_parts.append(out_part)
    hidden_all, dgate_all, dup_all, normed_mlp_all, grad_all = kept
    grad_normed_mlp = collect(back_parts)
    weight_grads = []
    for left, right in (
        (grad_all, hidden_all), (normed_mlp_all, dgate_all), (normed_mlp_all, dup_all)
    ):
        weight_grads.append(dot_tn(left, right).astype(bf16))
    grad_mlp = jnp.stack(weight_grads)
    grad_mlp = lax.psum_scatter(grad_mlp, "fsdp", scatter_dimension=1, tiled=True)
    grad_mlp = grad_mlp.astype(f32)
    grad_down = jnp.swapaxes(grad_mlp[0], 0, 1)
    grad_wgu = jnp.swapaxes(grad_mlp[1:], 0, 1)
    norm_part, grad_gain_mlp = norm_back(middle, inv_mlp, gains_all[1], grad_normed_mlp)
    grad_middle = out_cotangent + norm_part

    middle_blocks = spread(grad_middle.astype(bf16))
    do_parts = [dot_nt(block, w_out_all).astype(bf16) for block in middle_blocks]
    grad_attended = in_order(do_parts).reshape(row_count, kv_local, group_size, head_size)
    middle_all = in_order(middle_blocks)

    grad_wo = dot_tn(middle_all, attended).astype(bf16)

    out_totals = [after(out_parts[1 % ring], middle_blocks[-1]).astype(bf16)]
    for step in range(2, ring + 1):
        out_totals.append((shift(out_totals[-1]).astype(f32) + out_parts[step % ring]))
        if step < ring:
            out_totals[-1] = out_totals[-1].astype(bf16)
    output_rows = middle + out_totals[-1]

    attended_heads = attended.reshape(row_count, kv_local, group_size, head_size)
    grad_keys = jnp.zeros((row_count, kv_local, head_size), f32)
    grad_values = jnp.zeros((row_count, kv_local, head_size), f32)
    query_grads = []
    for block_index, block_start in enumerate(block_starts):
        block_stop = block_start + block_rows
        key_low, key_high = windows[block_index]
        grad_out = after(grad_attended[block_start:block_stop], out_totals[block_index])
        grad_query_block, grad_key_part, grad_value_part = attend_back(
            query_rows[block_start:block_stop],
            key_rows[key_low:key_high],
            value_rows[key_low:key_high],
            mask_list[block_index],
            total_list[block_index],
            attended_heads[block_start:block_stop],
            grad_out,
            score_scale,
        )
        query_grads.append(grad_query_block)
        pad_width = ((key_low, row_count - key_high), (0, 0), (0, 0))
        grad_keys = grad_keys + jnp.pad(grad_key_part, pad_width)
        grad_values = grad_values + jnp.pad(grad_value_part, pad_width)
    grad_query = (
        rotate(jnp.concatenate(query_grads, axis=0), cosine, sine_table, -1.0)
        .astype(bf16)
        .reshape(row_count, -1)
    )
    grad_keyval = (
        jnp.concatenate([rotate(grad_keys, cosine, sine_table, -1.0), grad_values], axis=-1)
        .astype(bf16)
        .reshape(row_count, -1)
    )
    grad_qkv = jnp.concatenate([grad_query, grad_keyval], axis=1)
    grad_qkv = after(grad_qkv, out_totals[-2])
    in_parts = [dot_nt(rows_of(grad_qkv, step), w_qkv) for step in range(ring)]
    grad_normed = collect(in_parts, output_rows)
    norm_part, _ = norm_back(residual, inv_attn, gains_all[0], grad_normed)
    grad_rows = grad_middle + norm_part

    grad_gain_attn = sum(
        jnp.sum(part * block.astype(f32) * pair[0], axis=0)
        for part, block, pair in zip(in_parts, input_blocks, normed_pairs)
    )
    grad_wqkv = dot_tn(normed_all, grad_qkv).astype(bf16)
    gain_columns = jnp.stack([grad_gain_attn, grad_gain_mlp], axis=1).astype(bf16)
    gain_columns = jnp.pad(gain_columns, ((0, 0), (0, 126)))
    packed = lax.psum_scatter(
        jnp.concatenate([grad_wqkv, grad_wo, gain_columns], axis=1),
        "fsdp", scatter_dimension=0, tiled=True,
    )
    packed = packed.astype(f32)
    qkv_width = grad_wqkv.shape[1]
    gain_start = qkv_width + grad_wo.shape[1]
    grad_wq = packed[:, :query_width]
    grad_wkv = packed[:, query_width:qkv_width].reshape(-1, kv_local, 2 * head_size)
    grad_wo = jnp.swapaxes(packed[:, qkv_width:gain_start], 0, 1)
    gain_part = packed[:, gain_start : gain_start + 2]
    gain_total = gain_part
    for distance in range(1, ring):
        gain_total = gain_total + lax.ppermute(
            gain_part, "tensor", [(i, (i + distance) % ring) for i in range(ring)]
        )
    return (
        output_rows,
        grad_rows,
        grad_wq[None],
        grad_wkv[None],
        grad_wo[None],
        grad_wgu[None],
        grad_down[None],
        gain_total.T[None],
    )


def solution(mesh):
    return jax.shard_map(
        per_device,
        mesh=mesh,
        in_specs=(
            P(("fsdp", "tensor"), None),
            P("fsdp", None),
            P(None, "fsdp", "tensor"),
            P(None, "fsdp", "tensor", None),
            P(None, "tensor", "fsdp"),
            P(None, "fsdp", None, "tensor"),
            P(None, "tensor", "fsdp"),
            P(None, None, "fsdp"),
            P(("fsdp", "tensor"), None),
        ),
        out_specs=(
            P(("fsdp", "tensor"), None),
            P(("fsdp", "tensor"), None),
            P(None, "fsdp", "tensor"),
            P(None, "fsdp", "tensor", None),
            P(None, "tensor", "fsdp"),
            P(None, "fsdp", None, "tensor"),
            P(None, "tensor", "fsdp"),
            P(None, None, "fsdp"),
        ),
        check_vma=False,
    )
```

```python
import functools

import jax
import jax.numpy as jnp
from jax import lax
from jax.experimental import pallas as pl
from jax.experimental.layout import Layout, with_layout_constraint
from jax.experimental.pallas import tpu as pltpu
from jax.sharding import PartitionSpec as P


MAXLEN = 512


NORM_EPSILON = 1e-05
ROPE_BASE = 500000.0


def norm_apply(residual, gain):
    inverse = lax.rsqrt(jnp.mean(residual * residual, axis=-1, keepdims=True) + NORM_EPSILON)
    return (inverse, (residual * inverse * gain.astype(jnp.float32)).astype(jnp.bfloat16))


def norm_back(residual, inverse, gain, grad_normed):
    scaled = grad_normed * gain.astype(jnp.float32)
    grad_gain = jnp.sum(grad_normed * residual * inverse, axis=0)
    grad_residual = inverse * scaled - residual * inverse * inverse * inverse * jnp.mean(
        scaled * residual, axis=-1, keepdims=True
    )
    return (grad_residual, grad_gain)


def rope_tables(doc_row, head_size):
    places = jnp.arange(doc_row.shape[0], dtype=jnp.int32)
    doc_start = jnp.concatenate([jnp.array([True]), doc_row[1:] != doc_row[:-1]])
    starts = lax.cummax(jnp.where(doc_start, places, 0), axis=0)
    exponent = jnp.arange(head_size // 2, dtype=jnp.float32) * (-2.0 / head_size)
    angles = (places - starts).astype(jnp.float32)[:, None] * jnp.power(ROPE_BASE, exponent)[
        None, :
    ]
    return (jnp.cos(angles), jnp.sin(angles))


def rotate(vectors, cosine, sine_table, direction_sign):
    half_size = vectors.shape[-1] // 2
    table_shape = (vectors.shape[0],) + (1,) * (vectors.ndim - 2) + (half_size,)
    cos_part = cosine.reshape(table_shape)
    sin_part = direction_sign * sine_table.reshape(table_shape)
    first_half = vectors[..., :half_size]
    second = vectors[..., half_size:]
    return jnp.concatenate(
        [first_half * cos_part - second * sin_part, second * cos_part + first_half * sin_part],
        axis=-1,
    )


def block_mask(doc_row, block_start, block_rows, key_low, key_high):
    places = jnp.arange(doc_row.shape[0], dtype=jnp.int32)
    own_docs = doc_row[block_start : block_start + block_rows]
    own_places = places[block_start : block_start + block_rows]
    return (own_docs[:, None] == doc_row[None, key_low:key_high]) & (
        places[None, key_low:key_high] <= own_places[:, None]
    )


def attend_block(query_rows, key_rows, value_rows, allowed, score_scale):
    scores = (
        jnp.einsum("qkgd,skd->kgqs", query_rows, key_rows, preferred_element_type=jnp.float32)
        * score_scale
    )
    scores = jnp.where(allowed[None, None], scores, -jnp.inf)
    row_max = jnp.max(scores, axis=-1, keepdims=True)
    log_total = row_max + jnp.log(jnp.sum(jnp.exp(scores - row_max), axis=-1, keepdims=True))
    probabilities = jnp.exp(scores - log_total).astype(jnp.bfloat16)
    attn_out = jnp.einsum(
        "kgqs,skd->qkgd", probabilities, value_rows, preferred_element_type=jnp.float32
    )
    return (attn_out.astype(jnp.bfloat16), log_total)


def attend_back(
    query_rows, key_rows, value_rows, allowed, log_total, out_rows, grad_out, score_scale
):
    scores = (
        jnp.einsum("qkgd,skd->kgqs", query_rows, key_rows, preferred_element_type=jnp.float32)
        * score_scale
    )
    scores = jnp.where(allowed[None, None], scores, -jnp.inf)
    probabilities = jnp.exp(scores - log_total)
    row_delta = jnp.einsum("qkgd,qkgd->kgq", grad_out, out_rows, preferred_element_type=jnp.float32)
    grad_probs = jnp.einsum(
        "qkgd,skd->kgqs", grad_out, value_rows, preferred_element_type=jnp.float32
    )
    grad_scores = (probabilities * (grad_probs - row_delta[..., None]) * score_scale).astype(
        jnp.bfloat16
    )
    grad_query = jnp.einsum(
        "kgqs,skd->qkgd", grad_scores, key_rows, preferred_element_type=jnp.float32
    )
    grad_key = jnp.einsum(
        "kgqs,qkgd->skd", grad_scores, query_rows, preferred_element_type=jnp.float32
    )
    grad_value = jnp.einsum(
        "kgqs,qkgd->skd",
        probabilities.astype(jnp.bfloat16),
        grad_out,
        preferred_element_type=jnp.float32,
    )
    return (grad_query, grad_key, grad_value)


def mlp_kernel(reused, *refs):
    x_ref, g_ref, w_ref = refs[:3]
    hidden_ref, dgu_ref, x_all_ref, g_all_ref, back_ref, out_ref = refs[3 + reused :]
    first = pl.program_id(0) == 0
    dims = (((1,), (1,)), ((), ()))
    x = x_ref[...]
    g = g_ref[...]
    w_gate = w_ref[0]
    w_up = w_ref[1]
    w_down = w_ref[2]
    tile = w_down.shape[1]
    gate = jnp.dot(x, w_gate, preferred_element_type=jnp.float32)
    up = jnp.dot(x, w_up, preferred_element_type=jnp.float32)
    grad_hidden = jnp.dot(g, w_down, preferred_element_type=jnp.float32)
    sigmoid_gate = 1.0 / (1.0 + jnp.exp(-gate))
    silu_gate = gate * sigmoid_gate
    hidden = (silu_gate * up).astype(jnp.bfloat16)
    dgate = (grad_hidden * up * sigmoid_gate * (1.0 + gate * (1.0 - sigmoid_gate))).astype(
        jnp.bfloat16
    )
    dup = (grad_hidden * silu_gate).astype(jnp.bfloat16)
    hidden_ref[...] = hidden
    dgu_ref[:, :tile] = dgate
    dgu_ref[:, tile:] = dup

    @pl.when(first)
    def _():
        x_all_ref[...] = x
        g_all_ref[...] = g
        out_ref[...] = jnp.zeros_like(out_ref)
        back_ref[...] = jnp.zeros_like(back_ref)

    out_ref[...] += lax.dot_general(hidden, w_down, dims, preferred_element_type=jnp.float32)
    back_ref[...] += lax.dot_general(
        dgate, w_gate, dims, preferred_element_type=jnp.float32
    ) + lax.dot_general(dup, w_up, dims, preferred_element_type=jnp.float32)


def mlp_tile(hidden_width):
    return min(512, hidden_width)


def mlp_block(step, ring, x, g, w_mlp, kept):
    rows, width = x.shape
    hidden_width = w_mlp.shape[2]
    tile = mlp_tile(hidden_width)
    bf16, f32 = jnp.bfloat16, jnp.float32
    wide = jax.ShapeDtypeStruct((ring * rows, hidden_width), bf16)
    pair = jax.ShapeDtypeStruct((ring * rows, 2 * hidden_width), bf16)
    whole = jax.ShapeDtypeStruct((ring * rows, width), bf16)
    part = jax.ShapeDtypeStruct((rows, width), f32)
    wide_spec = pl.BlockSpec((rows, tile), lambda t: (step, t))
    pair_spec = pl.BlockSpec((rows, 2 * tile), lambda t: (step, t))
    whole_spec = pl.BlockSpec((rows, width), lambda t: (step, 0))
    block_spec = pl.BlockSpec((rows, width), lambda t: (0, 0))
    reused = len(kept)
    return pl.pallas_call(
        functools.partial(mlp_kernel, reused),
        grid=(hidden_width // tile,),
        out_shape=(wide, pair, whole, whole, part, part),
        in_specs=[
            block_spec,
            block_spec,
            pl.BlockSpec((3, width, tile), lambda t: (0, 0, t)),
        ]
        + [pl.BlockSpec(memory_space=pl.ANY)] * reused,
        out_specs=(wide_spec, pair_spec, whole_spec, whole_spec, block_spec, block_spec),
        input_output_aliases={3 + i: i for i in range(reused)},
        cost_estimate=pl.CostEstimate(
            flops=12 * rows * width * hidden_width,
            bytes_accessed=6 * width * hidden_width + 12 * rows * width,
            transcendentals=rows * hidden_width,
        ),
        compiler_params=pltpu.CompilerParams(vmem_limit_bytes=44 << 20),
        name="mlp_block",
    )(x, g, w_mlp, *kept)


def per_device(
    block_input,
    doc_ids,
    w_query,
    w_keyval,
    w_attn_out,
    w_gate_up,
    w_down,
    norm_gains,
    out_cotangent,
):
    f32, bf16 = jnp.float32, jnp.bfloat16
    ring = lax.axis_size("tensor")
    place = lax.axis_index("tensor")
    ring_pairs = [(i, (i + 1) % ring) for i in range(ring)]
    doc_row = doc_ids[0]
    row_count = doc_row.shape[0]
    local_rows, _ = block_input.shape
    kv_local = w_keyval.shape[2]
    head_size = w_keyval.shape[3] // 2
    query_width = w_query.shape[2]
    group_size = query_width // (kv_local * head_size)
    block_rows = min(512, row_count)
    score_scale = head_size ** (-0.5)

    def row_major(array):
        return with_layout_constraint(array, Layout(tuple(range(array.ndim))))

    def dot(a, b):
        return jnp.dot(a, b, preferred_element_type=f32)

    def dot_nt(a, b):
        return lax.dot_general(a, b, (((1,), (1,)), ((), ())), preferred_element_type=f32)

    def dot_tn(a, b):
        return lax.dot_general(a, b, (((0,), (0,)), ((), ())), preferred_element_type=f32)

    def shift(rows):
        return lax.ppermute(rows, "tensor", ring_pairs)

    def after(value, gate):
        return lax.optimization_barrier((value, gate))[0]

    def block_start_of(step):
        return lax.rem(place - step + ring, ring) * local_rows

    def spread(rows):
        blocks = [rows]
        for _ in range(1, ring):
            blocks.append(shift(blocks[-1]))
        return blocks

    halves = 2
    half_rows = local_rows // halves

    def split(rows):
        return [rows[half * half_rows : (half + 1) * half_rows] for half in range(halves)]

    def spread_halves(rows):
        pieces = lax.optimization_barrier(split(rows))
        chains = [spread(piece) for piece in pieces]
        return [[chain[step] for chain in chains] for step in range(ring)]

    def in_order(blocks):
        first = blocks[0][0]
        whole = jnp.zeros((ring * local_rows,) + first.shape[1:], first.dtype)
        for step, pieces in enumerate(blocks):
            for half, piece in enumerate(pieces):
                whole = lax.dynamic_update_slice_in_dim(
                    whole, piece, block_start_of(step) + half * half_rows, 0
                )
        return whole

    def halves_of(whole, step):
        return [
            lax.dynamic_slice_in_dim(whole, block_start_of(step) + half * half_rows, half_rows, 0)
            for half in range(halves)
        ]

    def collect(parts):
        total = parts[1 % ring].astype(f32)
        for step in range(2, ring + 1):
            total = shift(total.astype(bf16)).astype(f32) + parts[step % ring]
        return total

    def collect_halves(parts):
        return jnp.concatenate(
            [collect([pieces[half] for pieces in parts]) for half in range(halves)],
            axis=0,
        )

    w_qkv_local = jnp.concatenate([w_query[0], w_keyval[0].reshape(w_keyval.shape[1], -1)], axis=1)
    w_qkv_local = row_major(w_qkv_local)
    w_mlp_local = jnp.stack([w_gate_up[0, :, 0], w_gate_up[0, :, 1], jnp.swapaxes(w_down[0], 0, 1)])
    w_qkv = row_major(lax.all_gather(w_qkv_local, "fsdp", axis=0, tiled=True))
    gains_all = lax.all_gather(norm_gains[0], "fsdp", axis=1, tiled=True)
    w_out_all = lax.all_gather(w_attn_out[0], "fsdp", axis=1, tiled=True)
    w_mlp = lax.all_gather(w_mlp_local, "fsdp", axis=1, tiled=True)

    cosine, sine_table = rope_tables(doc_row, head_size)
    block_starts = list(range(0, row_count, block_rows))
    windows = [
        (max(0, start - MAXLEN), start + block_rows) for start in block_starts
    ]
    mask_list = [
        block_mask(doc_row, start, block_rows, windows[index][0], windows[index][1])
        for index, start in enumerate(block_starts)
    ]

    input_blocks = spread_halves(block_input)
    grad_blocks = spread(after(out_cotangent.astype(bf16), input_blocks[-1]))
    normed_pairs = [
        [norm_apply(piece.astype(f32), gains_all[0]) for piece in pieces] for pieces in input_blocks
    ]
    residual = block_input.astype(f32)
    inv_attn = norm_apply(residual, gains_all[0])[0]
    normed_all = in_order([[pair[1] for pair in pairs] for pairs in normed_pairs])
    qkv = dot(normed_all, w_qkv)
    query_rows = rotate(
        qkv[:, :query_width].reshape(row_count, kv_local, group_size, head_size),
        cosine, sine_table, 1.0,
    ).astype(bf16)
    keyval = qkv[:, query_width:].reshape(row_count, kv_local, 2 * head_size)
    key_rows = rotate(keyval[..., :head_size], cosine, sine_table, 1.0).astype(bf16)
    value_rows = keyval[..., head_size:].astype(bf16)
    out_list = []
    total_list = []
    for block_index, block_start in enumerate(block_starts):
        key_low, key_high = windows[block_index]
        attend_inputs = (
            query_rows[block_start : block_start + block_rows],
            key_rows[key_low:key_high],
            value_rows[key_low:key_high],
        )
        if block_index > 0:
            attend_inputs = after(attend_inputs, out_list[-1])
        out_block, log_total = attend_block(
            *attend_inputs,
            mask_list[block_index],
            score_scale,
        )
        out_list.append(out_block)
        total_list.append(log_total)
    attended = jnp.concatenate(out_list, axis=0).reshape(row_count, -1)
    middle = residual + collect_halves(
        [[dot(piece, w_out_all) for piece in halves_of(attended, step)] for step in range(ring)],
    )
    inv_mlp, normed_mlp = norm_apply(middle, gains_all[1])

    normed_mlp_blocks = [normed_mlp]
    kept, back_parts, out_parts = (), [], []
    for step in range(ring):
        if step > 0:
            source = normed_mlp_blocks[-1]
            if step > 1:
                source = after(source, back_parts[step - 2])
            normed_mlp_blocks.append(shift(source))
        rows = normed_mlp_blocks[step]
        if step > 0:
            rows = after(rows, back_parts[step - 1])
        *kept, back_part, out_part = mlp_block(
            step, ring, rows, grad_blocks[step], w_mlp, tuple(kept)
        )
        back_parts.append(back_part)
        out_parts.append(out_part)
    hidden_all, dgu_all, normed_mlp_all, grad_all = kept
    grad_normed_mlp = collect(back_parts)
    grad_down = dot_tn(grad_all, hidden_all).astype(bf16)
    grad_wgu = dot_tn(normed_mlp_all, dgu_all).astype(bf16)
    grad_down = lax.psum_scatter(grad_down, "fsdp", scatter_dimension=0, tiled=True)
    grad_wgu = lax.psum_scatter(grad_wgu, "fsdp", scatter_dimension=0, tiled=True)
    grad_down = jnp.swapaxes(grad_down.astype(f32), 0, 1)
    tile = mlp_tile(w_mlp.shape[2])
    grad_wgu = grad_wgu.astype(f32).reshape(grad_wgu.shape[0], -1, 2, tile)
    grad_wgu = jnp.swapaxes(grad_wgu, 1, 2).reshape(grad_wgu.shape[0], 2, -1)
    norm_part, grad_gain_mlp = norm_back(middle, inv_mlp, gains_all[1], grad_normed_mlp)
    grad_middle = out_cotangent + norm_part

    middle_blocks = spread_halves(grad_middle.astype(bf16))
    do_parts = [
        [dot_nt(piece, w_out_all).astype(bf16) for piece in pieces] for pieces in middle_blocks
    ]
    grad_attended = in_order(do_parts).reshape(row_count, kv_local, group_size, head_size)
    middle_all = in_order(middle_blocks)

    grad_wo = dot_tn(middle_all, attended).astype(bf16)

    out_totals = [after(out_parts[1 % ring], middle_blocks[-1]).astype(bf16)]
    for step in range(2, ring + 1):
        out_totals.append((shift(out_totals[-1]).astype(f32) + out_parts[step % ring]))
        if step < ring:
            out_totals[-1] = out_totals[-1].astype(bf16)
    output_rows = middle + out_totals[-1]

    attended_heads = attended.reshape(row_count, kv_local, group_size, head_size)
    grad_keys = jnp.zeros((row_count, kv_local, head_size), f32)
    grad_values = jnp.zeros((row_count, kv_local, head_size), f32)
    query_grads = []
    for block_index, block_start in enumerate(block_starts):
        block_stop = block_start + block_rows
        key_low, key_high = windows[block_index]
        grad_out = after(grad_attended[block_start:block_stop], out_totals[block_index])
        grad_query_block, grad_key_part, grad_value_part = attend_back(
            query_rows[block_start:block_stop],
            key_rows[key_low:key_high],
            value_rows[key_low:key_high],
            mask_list[block_index],
            total_list[block_index],
            attended_heads[block_start:block_stop],
            grad_out,
            score_scale,
        )
        query_grads.append(grad_query_block)
        pad_width = ((key_low, row_count - key_high), (0, 0), (0, 0))
        grad_keys = grad_keys + jnp.pad(grad_key_part, pad_width)
        grad_values = grad_values + jnp.pad(grad_value_part, pad_width)
    grad_query = (
        rotate(jnp.concatenate(query_grads, axis=0), cosine, sine_table, -1.0)
        .astype(bf16)
        .reshape(row_count, -1)
    )
    grad_keyval = (
        jnp.concatenate([rotate(grad_keys, cosine, sine_table, -1.0), grad_values], axis=-1)
        .astype(bf16)
        .reshape(row_count, -1)
    )
    grad_qkv = jnp.concatenate([grad_query, grad_keyval], axis=1)
    grad_qkv = after(grad_qkv, out_totals[-2])
    in_parts = [
        [dot_nt(piece, w_qkv) for piece in halves_of(grad_qkv, step)] for step in range(ring)
    ]
    grad_normed = collect_halves(in_parts)
    norm_part, _ = norm_back(residual, inv_attn, gains_all[0], grad_normed)
    grad_rows = grad_middle + norm_part

    grad_wqkv = dot_tn(normed_all, grad_qkv)
    grad_gain_attn = jnp.sum(grad_wqkv * w_qkv.astype(f32), axis=1) / gains_all[0].astype(f32)
    grad_wqkv = grad_wqkv.astype(bf16)
    gain_columns = jnp.stack([grad_gain_attn, grad_gain_mlp], axis=1).astype(bf16)
    gain_columns = jnp.pad(gain_columns, ((0, 0), (0, 126)))
    packed = lax.psum_scatter(
        jnp.concatenate([grad_wqkv, grad_wo, gain_columns], axis=1),
        "fsdp", scatter_dimension=0, tiled=True,
    )
    packed = packed.astype(f32)
    qkv_width = grad_wqkv.shape[1]
    gain_start = qkv_width + grad_wo.shape[1]
    grad_wq = packed[:, :query_width]
    grad_wkv = packed[:, query_width:qkv_width].reshape(-1, kv_local, 2 * head_size)
    grad_wo = jnp.swapaxes(packed[:, qkv_width:gain_start], 0, 1)
    gain_part = packed[:, gain_start : gain_start + 2]
    gain_total = gain_part
    for distance in range(1, ring):
        gain_total = gain_total + lax.ppermute(
            gain_part, "tensor", [(i, (i + distance) % ring) for i in range(ring)]
        )
    return (
        output_rows,
        grad_rows,
        grad_wq[None],
        grad_wkv[None],
        grad_wo[None],
        grad_wgu[None],
        grad_down[None],
        gain_total.T[None],
    )


def solution(mesh):
    return jax.shard_map(
        per_device,
        mesh=mesh,
        in_specs=(
            P(("fsdp", "tensor"), None),
            P("fsdp", None),
            P(None, "fsdp", "tensor"),
            P(None, "fsdp", "tensor", None),
            P(None, "tensor", "fsdp"),
            P(None, "fsdp", None, "tensor"),
            P(None, "tensor", "fsdp"),
            P(None, None, "fsdp"),
            P(("fsdp", "tensor"), None),
        ),
        out_specs=(
            P(("fsdp", "tensor"), None),
            P(("fsdp", "tensor"), None),
            P(None, "fsdp", "tensor"),
            P(None, "fsdp", "tensor", None),
            P(None, "tensor", "fsdp"),
            P(None, "fsdp", None, "tensor"),
            P(None, "tensor", "fsdp"),
            P(None, None, "fsdp"),
        ),
        check_vma=False,
    )
```

```python
import functools

import jax
import jax.numpy as jnp
from jax import lax
from jax.experimental import pallas as pl
from jax.experimental.layout import Layout, with_layout_constraint
from jax.experimental.pallas import tpu as pltpu
from jax.sharding import PartitionSpec as P


MAXLEN = 512


NORM_EPSILON = 1e-05
ROPE_BASE = 500000.0


def norm_apply(residual, gain):
    inverse = lax.rsqrt(jnp.mean(residual * residual, axis=-1, keepdims=True) + NORM_EPSILON)
    return (inverse, (residual * inverse * gain.astype(jnp.float32)).astype(jnp.bfloat16))


def norm_back(residual, inverse, gain, grad_normed):
    scaled = grad_normed * gain.astype(jnp.float32)
    grad_gain = jnp.sum(grad_normed * residual * inverse, axis=0)
    grad_residual = inverse * scaled - residual * inverse * inverse * inverse * jnp.mean(
        scaled * residual, axis=-1, keepdims=True
    )
    return (grad_residual, grad_gain)


def rope_tables(doc_row, head_size):
    places = jnp.arange(doc_row.shape[0], dtype=jnp.int32)
    doc_start = jnp.concatenate([jnp.array([True]), doc_row[1:] != doc_row[:-1]])
    starts = lax.cummax(jnp.where(doc_start, places, 0), axis=0)
    exponent = jnp.arange(head_size // 2, dtype=jnp.float32) * (-2.0 / head_size)
    angles = (places - starts).astype(jnp.float32)[:, None] * jnp.power(ROPE_BASE, exponent)[
        None, :
    ]
    return (jnp.cos(angles), jnp.sin(angles))


def rotate(vectors, cosine, sine_table, direction_sign):
    half_size = vectors.shape[-1] // 2
    table_shape = (vectors.shape[0],) + (1,) * (vectors.ndim - 2) + (half_size,)
    cos_part = cosine.reshape(table_shape)
    sin_part = direction_sign * sine_table.reshape(table_shape)
    first_half = vectors[..., :half_size]
    second = vectors[..., half_size:]
    return jnp.concatenate(
        [first_half * cos_part - second * sin_part, second * cos_part + first_half * sin_part],
        axis=-1,
    )


def block_mask(doc_row, block_start, block_rows, key_low, key_high):
    places = jnp.arange(doc_row.shape[0], dtype=jnp.int32)
    own_docs = doc_row[block_start : block_start + block_rows]
    own_places = places[block_start : block_start + block_rows]
    return (own_docs[:, None] == doc_row[None, key_low:key_high]) & (
        places[None, key_low:key_high] <= own_places[:, None]
    )


def attend_block(query_rows, key_rows, value_rows, allowed, score_scale):
    scores = (
        jnp.einsum("qkgd,skd->kgqs", query_rows, key_rows, preferred_element_type=jnp.float32)
        * score_scale
    )
    scores = jnp.where(allowed[None, None], scores, -jnp.inf)
    row_max = jnp.max(scores, axis=-1, keepdims=True)
    log_total = row_max + jnp.log(jnp.sum(jnp.exp(scores - row_max), axis=-1, keepdims=True))
    probabilities = jnp.exp(scores - log_total).astype(jnp.bfloat16)
    attn_out = jnp.einsum(
        "kgqs,skd->qkgd", probabilities, value_rows, preferred_element_type=jnp.float32
    )
    return (attn_out.astype(jnp.bfloat16), log_total)


def attend_back(
    query_rows, key_rows, value_rows, allowed, log_total, out_rows, grad_out, score_scale
):
    scores = (
        jnp.einsum("qkgd,skd->kgqs", query_rows, key_rows, preferred_element_type=jnp.float32)
        * score_scale
    )
    scores = jnp.where(allowed[None, None], scores, -jnp.inf)
    probabilities = jnp.exp(scores - log_total)
    row_delta = jnp.einsum("qkgd,qkgd->kgq", grad_out, out_rows, preferred_element_type=jnp.float32)
    grad_probs = jnp.einsum(
        "qkgd,skd->kgqs", grad_out, value_rows, preferred_element_type=jnp.float32
    )
    grad_scores = (probabilities * (grad_probs - row_delta[..., None]) * score_scale).astype(
        jnp.bfloat16
    )
    grad_query = jnp.einsum(
        "kgqs,skd->qkgd", grad_scores, key_rows, preferred_element_type=jnp.float32
    )
    grad_key = jnp.einsum(
        "kgqs,qkgd->skd", grad_scores, query_rows, preferred_element_type=jnp.float32
    )
    grad_value = jnp.einsum(
        "kgqs,qkgd->skd",
        probabilities.astype(jnp.bfloat16),
        grad_out,
        preferred_element_type=jnp.float32,
    )
    return (grad_query, grad_key, grad_value)


def mlp_kernel(reused, *refs):
    x_ref, g_ref, w_ref = refs[:3]
    hidden_ref, dgu_ref, x_all_ref, g_all_ref, back_ref, out_ref = refs[3 + reused :]
    first = pl.program_id(0) == 0
    dims = (((1,), (1,)), ((), ()))
    x = x_ref[...]
    g = g_ref[...]
    w_gate = w_ref[0]
    w_up = w_ref[1]
    w_down = w_ref[2]
    tile = w_down.shape[1]
    gate = jnp.dot(x, w_gate, preferred_element_type=jnp.float32)
    up = jnp.dot(x, w_up, preferred_element_type=jnp.float32)
    grad_hidden = jnp.dot(g, w_down, preferred_element_type=jnp.float32)
    sigmoid_gate = 1.0 / (1.0 + jnp.exp(-gate))
    silu_gate = gate * sigmoid_gate
    hidden = (silu_gate * up).astype(jnp.bfloat16)
    dgate = (grad_hidden * up * sigmoid_gate * (1.0 + gate * (1.0 - sigmoid_gate))).astype(
        jnp.bfloat16
    )
    dup = (grad_hidden * silu_gate).astype(jnp.bfloat16)
    hidden_ref[...] = hidden
    dgu_ref[:, :tile] = dgate
    dgu_ref[:, tile:] = dup

    @pl.when(first)
    def _():
        x_all_ref[...] = x
        g_all_ref[...] = g
        out_ref[...] = jnp.zeros_like(out_ref)
        back_ref[...] = jnp.zeros_like(back_ref)

    out_ref[...] += lax.dot_general(hidden, w_down, dims, preferred_element_type=jnp.float32)
    back_ref[...] += lax.dot_general(
        dgate, w_gate, dims, preferred_element_type=jnp.float32
    ) + lax.dot_general(dup, w_up, dims, preferred_element_type=jnp.float32)


def mlp_tile(hidden_width):
    return min(512, hidden_width)


def mlp_block(step, ring, x, g, w_mlp, kept):
    rows, width = x.shape
    hidden_width = w_mlp.shape[2]
    tile = mlp_tile(hidden_width)
    bf16, f32 = jnp.bfloat16, jnp.float32
    wide = jax.ShapeDtypeStruct((ring * rows, hidden_width), bf16)
    pair = jax.ShapeDtypeStruct((ring * rows, 2 * hidden_width), bf16)
    whole = jax.ShapeDtypeStruct((ring * rows, width), bf16)
    part = jax.ShapeDtypeStruct((rows, width), f32)
    wide_spec = pl.BlockSpec((rows, tile), lambda t: (step, t))
    pair_spec = pl.BlockSpec((rows, 2 * tile), lambda t: (step, t))
    whole_spec = pl.BlockSpec((rows, width), lambda t: (step, 0))
    block_spec = pl.BlockSpec((rows, width), lambda t: (0, 0))
    reused = len(kept)
    return pl.pallas_call(
        functools.partial(mlp_kernel, reused),
        grid=(hidden_width // tile,),
        out_shape=(wide, pair, whole, whole, part, part),
        in_specs=[
            block_spec,
            block_spec,
            pl.BlockSpec((3, width, tile), lambda t: (0, 0, t)),
        ]
        + [pl.BlockSpec(memory_space=pl.ANY)] * reused,
        out_specs=(wide_spec, pair_spec, whole_spec, whole_spec, block_spec, block_spec),
        input_output_aliases={3 + i: i for i in range(reused)},
        cost_estimate=pl.CostEstimate(
            flops=12 * rows * width * hidden_width,
            bytes_accessed=6 * width * hidden_width + 12 * rows * width,
            transcendentals=rows * hidden_width,
        ),
        compiler_params=pltpu.CompilerParams(vmem_limit_bytes=44 << 20),
        name="mlp_block",
    )(x, g, w_mlp, *kept)


def per_device(
    block_input,
    doc_ids,
    w_query,
    w_keyval,
    w_attn_out,
    w_gate_up,
    w_down,
    norm_gains,
    out_cotangent,
):
    f32, bf16 = jnp.float32, jnp.bfloat16
    ring = lax.axis_size("tensor")
    place = lax.axis_index("tensor")
    ring_pairs = [(i, (i + 1) % ring) for i in range(ring)]
    doc_row = doc_ids[0]
    row_count = doc_row.shape[0]
    local_rows, _ = block_input.shape
    kv_local = w_keyval.shape[2]
    head_size = w_keyval.shape[3] // 2
    query_width = w_query.shape[2]
    group_size = query_width // (kv_local * head_size)
    block_rows = min(512, row_count)
    score_scale = head_size ** (-0.5)

    def row_major(array):
        return with_layout_constraint(array, Layout(tuple(range(array.ndim))))

    def dot(a, b):
        return jnp.dot(a, b, preferred_element_type=f32)

    def dot_nt(a, b):
        return lax.dot_general(a, b, (((1,), (1,)), ((), ())), preferred_element_type=f32)

    def dot_tn(a, b):
        return lax.dot_general(a, b, (((0,), (0,)), ((), ())), preferred_element_type=f32)

    def shift(rows):
        return lax.ppermute(rows, "tensor", ring_pairs)

    def after(value, gate):
        return lax.optimization_barrier((value, gate))[0]

    def block_start_of(step):
        return lax.rem(place - step + ring, ring) * local_rows

    def spread(rows):
        blocks = [rows]
        for _ in range(1, ring):
            blocks.append(shift(blocks[-1]))
        return blocks

    halves = 2
    half_rows = local_rows // halves

    def split(rows):
        return [rows[half * half_rows : (half + 1) * half_rows] for half in range(halves)]

    def spread_halves(rows):
        pieces = lax.optimization_barrier(split(rows))
        chains = [spread(piece) for piece in pieces]
        return [[chain[step] for chain in chains] for step in range(ring)]

    def in_order(blocks):
        first = blocks[0][0]
        whole = jnp.zeros((ring * local_rows,) + first.shape[1:], first.dtype)
        for step, pieces in enumerate(blocks):
            for half, piece in enumerate(pieces):
                whole = lax.dynamic_update_slice_in_dim(
                    whole, piece, block_start_of(step) + half * half_rows, 0
                )
        return whole

    def halves_of(whole, step):
        return [
            lax.dynamic_slice_in_dim(whole, block_start_of(step) + half * half_rows, half_rows, 0)
            for half in range(halves)
        ]

    def collect(parts):
        total = parts[1 % ring].astype(f32)
        for step in range(2, ring + 1):
            total = shift(total.astype(bf16)).astype(f32) + parts[step % ring]
        return total

    def collect_halves(parts):
        return jnp.concatenate(
            [collect([pieces[half] for pieces in parts]) for half in range(halves)],
            axis=0,
        )

    w_qkv_local = jnp.concatenate([w_query[0], w_keyval[0].reshape(w_keyval.shape[1], -1)], axis=1)
    w_qkv_local = row_major(w_qkv_local)
    w_mlp_local = jnp.stack([w_gate_up[0, :, 0], w_gate_up[0, :, 1], jnp.swapaxes(w_down[0], 0, 1)])
    w_qkv = row_major(lax.all_gather(w_qkv_local, "fsdp", axis=0, tiled=True))
    gains_all = lax.all_gather(norm_gains[0], "fsdp", axis=1, tiled=True)
    w_out_all = lax.all_gather(w_attn_out[0], "fsdp", axis=1, tiled=True)
    w_mlp = lax.all_gather(w_mlp_local, "fsdp", axis=1, tiled=True)

    cosine, sine_table = rope_tables(doc_row, head_size)
    block_starts = list(range(0, row_count, block_rows))
    windows = [
        (max(0, start - MAXLEN), start + block_rows) for start in block_starts
    ]
    mask_list = [
        block_mask(doc_row, start, block_rows, windows[index][0], windows[index][1])
        for index, start in enumerate(block_starts)
    ]

    input_blocks = spread_halves(block_input)
    grad_blocks = spread(after(out_cotangent.astype(bf16), input_blocks[-1]))
    normed_pairs = []
    for pieces in input_blocks:
        normed_pairs.append([norm_apply(piece.astype(f32), gains_all[0]) for piece in pieces])
    residual = block_input.astype(f32)
    inv_attn = norm_apply(residual, gains_all[0])[0]
    normed_all = in_order([[pair[1] for pair in pairs] for pairs in normed_pairs])
    qkv = dot(normed_all, w_qkv)
    query_rows = rotate(
        qkv[:, :query_width].reshape(row_count, kv_local, group_size, head_size),
        cosine, sine_table, 1.0,
    ).astype(bf16)
    keyval = qkv[:, query_width:].reshape(row_count, kv_local, 2 * head_size)
    key_rows = rotate(keyval[..., :head_size], cosine, sine_table, 1.0).astype(bf16)
    value_rows = keyval[..., head_size:].astype(bf16)
    out_list = []
    total_list = []
    for block_index, block_start in enumerate(block_starts):
        key_low, key_high = windows[block_index]
        attend_inputs = (
            query_rows[block_start : block_start + block_rows],
            key_rows[key_low:key_high],
            value_rows[key_low:key_high],
        )
        if block_index > 0:
            attend_inputs = after(attend_inputs, out_list[-1])
        out_block, log_total = attend_block(
            *attend_inputs,
            mask_list[block_index],
            score_scale,
        )
        out_list.append(out_block)
        total_list.append(log_total)
    attended = jnp.concatenate(out_list, axis=0).reshape(row_count, -1)
    middle = residual + collect_halves(
        [[dot(piece, w_out_all) for piece in halves_of(attended, step)] for step in range(ring)],
    )
    inv_mlp, normed_mlp = norm_apply(middle, gains_all[1])

    normed_mlp_blocks = [normed_mlp]
    kept, back_parts, out_parts = (), [], []
    for step in range(ring):
        if step > 0:
            source = normed_mlp_blocks[-1]
            if step > 1:
                source = after(source, back_parts[step - 2])
            normed_mlp_blocks.append(shift(source))
        rows = normed_mlp_blocks[step]
        if step > 0:
            rows = after(rows, back_parts[step - 1])
        *kept, back_part, out_part = mlp_block(
            step, ring, rows, grad_blocks[step], w_mlp, tuple(kept)
        )
        back_parts.append(back_part)
        out_parts.append(out_part)
    hidden_all, dgu_all, normed_mlp_all, grad_all = kept
    grad_normed_mlp = collect(back_parts)
    grad_down = dot_tn(grad_all, hidden_all).astype(bf16)
    grad_wgu = dot_tn(normed_mlp_all, dgu_all).astype(bf16)
    grad_down = lax.psum_scatter(grad_down, "fsdp", scatter_dimension=0, tiled=True)
    grad_wgu = lax.psum_scatter(grad_wgu, "fsdp", scatter_dimension=0, tiled=True)
    grad_down = jnp.swapaxes(grad_down.astype(f32), 0, 1)
    tile = mlp_tile(w_mlp.shape[2])
    grad_wgu = grad_wgu.astype(f32).reshape(grad_wgu.shape[0], -1, 2, tile)
    grad_wgu = jnp.swapaxes(grad_wgu, 1, 2).reshape(grad_wgu.shape[0], 2, -1)
    gain_mlp_part = jnp.sum(grad_wgu * w_gate_up[0].astype(f32), axis=(1, 2))
    norm_part, _ = norm_back(middle, inv_mlp, gains_all[1], grad_normed_mlp)
    grad_middle = out_cotangent + norm_part

    middle_blocks = [[block] for block in spread(grad_middle.astype(bf16))]
    do_parts = [
        [dot_nt(piece, w_out_all).astype(bf16) for piece in pieces] for pieces in middle_blocks
    ]
    grad_attended = in_order(do_parts).reshape(row_count, kv_local, group_size, head_size)
    middle_all = in_order(middle_blocks)

    grad_wo = dot_tn(middle_all, attended).astype(bf16)

    out_totals = [after(out_parts[1 % ring], middle_blocks[-1]).astype(bf16)]
    for step in range(2, ring + 1):
        source = out_totals[-1]
        if step == ring:
            source = after(source, (grad_wgu, grad_down, gain_mlp_part))
        out_totals.append((shift(source).astype(f32) + out_parts[step % ring]))
        if step < ring:
            out_totals[-1] = out_totals[-1].astype(bf16)
    output_rows = middle + out_totals[-1]

    attended_heads = attended.reshape(row_count, kv_local, group_size, head_size)
    grad_keys = jnp.zeros((row_count, kv_local, head_size), f32)
    grad_values = jnp.zeros((row_count, kv_local, head_size), f32)
    query_grads = []
    for block_index, block_start in enumerate(block_starts):
        block_stop = block_start + block_rows
        key_low, key_high = windows[block_index]
        grad_out = after(grad_attended[block_start:block_stop], out_totals[block_index])
        grad_query_block, grad_key_part, grad_value_part = attend_back(
            query_rows[block_start:block_stop],
            key_rows[key_low:key_high],
            value_rows[key_low:key_high],
            mask_list[block_index],
            total_list[block_index],
            attended_heads[block_start:block_stop],
            grad_out,
            score_scale,
        )
        query_grads.append(grad_query_block)
        pad_width = ((key_low, row_count - key_high), (0, 0), (0, 0))
        grad_keys = grad_keys + jnp.pad(grad_key_part, pad_width)
        grad_values = grad_values + jnp.pad(grad_value_part, pad_width)
    grad_query = (
        rotate(jnp.concatenate(query_grads, axis=0), cosine, sine_table, -1.0)
        .astype(bf16)
        .reshape(row_count, -1)
    )
    grad_keyval = (
        jnp.concatenate([rotate(grad_keys, cosine, sine_table, -1.0), grad_values], axis=-1)
        .astype(bf16)
        .reshape(row_count, -1)
    )
    grad_qkv = jnp.concatenate([grad_query, grad_keyval], axis=1)
    grad_qkv = after(grad_qkv, out_totals[-2])
    in_parts = [
        [dot_nt(piece, w_qkv) for piece in halves_of(grad_qkv, step)] for step in range(ring)
    ]
    grad_normed = collect_halves(in_parts)
    norm_part, _ = norm_back(residual, inv_attn, gains_all[0], grad_normed)
    grad_rows = grad_middle + norm_part

    grad_wqkv = dot_tn(normed_all, grad_qkv)
    grad_wqkv = grad_wqkv.astype(bf16)
    packed = lax.psum_scatter(
        jnp.concatenate([grad_wqkv, grad_wo], axis=1),
        "fsdp", scatter_dimension=0, tiled=True,
    )
    packed = packed.astype(f32)
    qkv_width = grad_wqkv.shape[1]
    grad_wq = packed[:, :query_width]
    grad_wkv = packed[:, query_width:qkv_width].reshape(-1, kv_local, 2 * head_size)
    grad_wo = jnp.swapaxes(packed[:, qkv_width:], 0, 1)
    gain_attn_part = jnp.sum(packed[:, :qkv_width] * w_qkv_local.astype(f32), axis=1)
    gain_part = jnp.stack([gain_attn_part, gain_mlp_part]) / norm_gains[0].astype(f32)
    gain_total = gain_part
    for distance in range(1, ring):
        gain_total = gain_total + lax.ppermute(
            gain_part, "tensor", [(i, (i + distance) % ring) for i in range(ring)]
        )
    return (
        output_rows,
        grad_rows,
        grad_wq[None],
        grad_wkv[None],
        grad_wo[None],
        grad_wgu[None],
        grad_down[None],
        gain_total[None],
    )


def solution(mesh):
    return jax.shard_map(
        per_device,
        mesh=mesh,
        in_specs=(
            P(("fsdp", "tensor"), None),
            P("fsdp", None),
            P(None, "fsdp", "tensor"),
            P(None, "fsdp", "tensor", None),
            P(None, "tensor", "fsdp"),
            P(None, "fsdp", None, "tensor"),
            P(None, "tensor", "fsdp"),
            P(None, None, "fsdp"),
            P(("fsdp", "tensor"), None),
        ),
        out_specs=(
            P(("fsdp", "tensor"), None),
            P(("fsdp", "tensor"), None),
            P(None, "fsdp", "tensor"),
            P(None, "fsdp", "tensor", None),
            P(None, "tensor", "fsdp"),
            P(None, "fsdp", None, "tensor"),
            P(None, "tensor", "fsdp"),
            P(None, None, "fsdp"),
        ),
        check_vma=False,
    )
```

```python
import functools

import jax
import jax.numpy as jnp
from jax import lax
from jax.experimental import pallas as pl
from jax.experimental.layout import Layout, with_layout_constraint
from jax.experimental.pallas import tpu as pltpu
from jax.sharding import PartitionSpec as P


MAXLEN = 512


NORM_EPSILON = 1e-05
ROPE_BASE = 500000.0


def norm_apply(residual, gain):
    inverse = lax.rsqrt(jnp.mean(residual * residual, axis=-1, keepdims=True) + NORM_EPSILON)
    return (inverse, (residual * inverse * gain.astype(jnp.float32)).astype(jnp.bfloat16))


def norm_back(residual, inverse, gain, grad_normed):
    scaled = grad_normed * gain.astype(jnp.float32)
    grad_gain = jnp.sum(grad_normed * residual * inverse, axis=0)
    grad_residual = inverse * scaled - residual * inverse * inverse * inverse * jnp.mean(
        scaled * residual, axis=-1, keepdims=True
    )
    return (grad_residual, grad_gain)


def rope_tables(doc_row, head_size):
    places = jnp.arange(doc_row.shape[0], dtype=jnp.int32)
    doc_start = jnp.concatenate([jnp.array([True]), doc_row[1:] != doc_row[:-1]])
    starts = lax.cummax(jnp.where(doc_start, places, 0), axis=0)
    exponent = jnp.arange(head_size // 2, dtype=jnp.float32) * (-2.0 / head_size)
    angles = (places - starts).astype(jnp.float32)[:, None] * jnp.power(ROPE_BASE, exponent)[
        None, :
    ]
    return (jnp.cos(angles), jnp.sin(angles))


def rotate(vectors, cosine, sine_table, direction_sign):
    half_size = vectors.shape[-1] // 2
    table_shape = (vectors.shape[0],) + (1,) * (vectors.ndim - 2) + (half_size,)
    cos_part = cosine.reshape(table_shape)
    sin_part = direction_sign * sine_table.reshape(table_shape)
    first_half = vectors[..., :half_size]
    second = vectors[..., half_size:]
    return jnp.concatenate(
        [first_half * cos_part - second * sin_part, second * cos_part + first_half * sin_part],
        axis=-1,
    )


def block_mask(doc_row, block_start, block_rows, key_low, key_high):
    places = jnp.arange(doc_row.shape[0], dtype=jnp.int32)
    own_docs = doc_row[block_start : block_start + block_rows]
    own_places = places[block_start : block_start + block_rows]
    return (own_docs[:, None] == doc_row[None, key_low:key_high]) & (
        places[None, key_low:key_high] <= own_places[:, None]
    )


def attend_block(query_rows, key_rows, value_rows, allowed, score_scale):
    scores = (
        jnp.einsum("qkgd,skd->kgqs", query_rows, key_rows, preferred_element_type=jnp.float32)
        * score_scale
    )
    scores = jnp.where(allowed[None, None], scores, -jnp.inf)
    row_max = jnp.max(scores, axis=-1, keepdims=True)
    log_total = row_max + jnp.log(jnp.sum(jnp.exp(scores - row_max), axis=-1, keepdims=True))
    probabilities = jnp.exp(scores - log_total).astype(jnp.bfloat16)
    attn_out = jnp.einsum(
        "kgqs,skd->qkgd", probabilities, value_rows, preferred_element_type=jnp.float32
    )
    return (attn_out.astype(jnp.bfloat16), log_total)


def attend_back(
    query_rows, key_rows, value_rows, allowed, log_total, out_rows, grad_out, score_scale
):
    scores = (
        jnp.einsum("qkgd,skd->kgqs", query_rows, key_rows, preferred_element_type=jnp.float32)
        * score_scale
    )
    scores = jnp.where(allowed[None, None], scores, -jnp.inf)
    probabilities = jnp.exp(scores - log_total)
    row_delta = jnp.einsum("qkgd,qkgd->kgq", grad_out, out_rows, preferred_element_type=jnp.float32)
    grad_probs = jnp.einsum(
        "qkgd,skd->kgqs", grad_out, value_rows, preferred_element_type=jnp.float32
    )
    grad_scores = (probabilities * (grad_probs - row_delta[..., None]) * score_scale).astype(
        jnp.bfloat16
    )
    grad_query = jnp.einsum(
        "kgqs,skd->qkgd", grad_scores, key_rows, preferred_element_type=jnp.float32
    )
    grad_key = jnp.einsum(
        "kgqs,qkgd->skd", grad_scores, query_rows, preferred_element_type=jnp.float32
    )
    grad_value = jnp.einsum(
        "kgqs,qkgd->skd",
        probabilities.astype(jnp.bfloat16),
        grad_out,
        preferred_element_type=jnp.float32,
    )
    return (grad_query, grad_key, grad_value)


def mlp_kernel(reused, *refs):
    x_ref, g_ref, w_ref = refs[:3]
    right_ref, left_ref, back_ref, out_ref = refs[3 + reused :]
    first = pl.program_id(0) == 0
    dims = (((1,), (1,)), ((), ()))
    x = x_ref[...]
    g = g_ref[...]
    w_gate = w_ref[0]
    w_up = w_ref[1]
    w_down = w_ref[2]
    gate = jnp.dot(x, w_gate, preferred_element_type=jnp.float32)
    up = jnp.dot(x, w_up, preferred_element_type=jnp.float32)
    grad_hidden = jnp.dot(g, w_down, preferred_element_type=jnp.float32)
    sigmoid_gate = 1.0 / (1.0 + jnp.exp(-gate))
    silu_gate = gate * sigmoid_gate
    hidden = (silu_gate * up).astype(jnp.bfloat16)
    dgate = (grad_hidden * up * sigmoid_gate * (1.0 + gate * (1.0 - sigmoid_gate))).astype(
        jnp.bfloat16
    )
    dup = (grad_hidden * silu_gate).astype(jnp.bfloat16)
    right_ref[0] = hidden
    right_ref[1] = dgate
    right_ref[2] = dup

    @pl.when(first)
    def _():
        left_ref[0] = g
        left_ref[1] = x
        left_ref[2] = x
        out_ref[...] = jnp.zeros_like(out_ref)
        back_ref[...] = jnp.zeros_like(back_ref)

    out_ref[...] += lax.dot_general(hidden, w_down, dims, preferred_element_type=jnp.float32)
    back_ref[...] += lax.dot_general(
        dgate, w_gate, dims, preferred_element_type=jnp.float32
    ) + lax.dot_general(dup, w_up, dims, preferred_element_type=jnp.float32)


def mlp_block(step, ring, x, g, w_mlp, kept):
    rows, width = x.shape
    hidden_width = w_mlp.shape[2]
    tile = min(512, hidden_width)
    bf16, f32 = jnp.bfloat16, jnp.float32
    right = jax.ShapeDtypeStruct((3, ring * rows, hidden_width), bf16)
    left = jax.ShapeDtypeStruct((3, ring * rows, width), bf16)
    part = jax.ShapeDtypeStruct((rows, width), f32)
    right_spec = pl.BlockSpec((3, rows, tile), lambda t: (0, step, t))
    left_spec = pl.BlockSpec((3, rows, width), lambda t: (0, step, 0))
    block_spec = pl.BlockSpec((rows, width), lambda t: (0, 0))
    reused = len(kept)
    return pl.pallas_call(
        functools.partial(mlp_kernel, reused),
        grid=(hidden_width // tile,),
        out_shape=(right, left, part, part),
        in_specs=[
            block_spec,
            block_spec,
            pl.BlockSpec((3, width, tile), lambda t: (0, 0, t)),
        ]
        + [pl.BlockSpec(memory_space=pl.ANY)] * reused,
        out_specs=(right_spec, left_spec, block_spec, block_spec),
        input_output_aliases={3 + i: i for i in range(reused)},
        cost_estimate=pl.CostEstimate(
            flops=12 * rows * width * hidden_width,
            bytes_accessed=6 * width * hidden_width + 12 * rows * width,
            transcendentals=rows * hidden_width,
        ),
        compiler_params=pltpu.CompilerParams(vmem_limit_bytes=44 << 20),
        name="mlp_block",
    )(x, g, w_mlp, *kept)


def per_device(
    block_input,
    doc_ids,
    w_query,
    w_keyval,
    w_attn_out,
    w_gate_up,
    w_down,
    norm_gains,
    out_cotangent,
):
    f32, bf16 = jnp.float32, jnp.bfloat16
    ring = lax.axis_size("tensor")
    place = lax.axis_index("tensor")
    ring_pairs = [(i, (i + 1) % ring) for i in range(ring)]
    doc_row = doc_ids[0]
    row_count = doc_row.shape[0]
    local_rows, _ = block_input.shape
    kv_local = w_keyval.shape[2]
    head_size = w_keyval.shape[3] // 2
    query_width = w_query.shape[2]
    group_size = query_width // (kv_local * head_size)
    block_rows = min(512, row_count)
    score_scale = head_size ** (-0.5)

    def row_major(array):
        return with_layout_constraint(array, Layout(tuple(range(array.ndim))))

    def dot(a, b):
        return jnp.dot(a, b, preferred_element_type=f32)

    def dot_nt(a, b):
        return lax.dot_general(a, b, (((1,), (1,)), ((), ())), preferred_element_type=f32)

    def dot_tn(a, b):
        return lax.dot_general(a, b, (((0,), (0,)), ((), ())), preferred_element_type=f32)

    def shift(rows):
        return lax.ppermute(rows, "tensor", ring_pairs)

    def after(value, gate):
        return lax.optimization_barrier((value, gate))[0]

    def block_start_of(step):
        return lax.rem(place - step + ring, ring) * local_rows

    def spread(rows):
        blocks = [rows]
        for _ in range(1, ring):
            blocks.append(shift(blocks[-1]))
        return blocks

    halves = 2
    half_rows = local_rows // halves

    def split(rows):
        return [rows[half * half_rows : (half + 1) * half_rows] for half in range(halves)]

    def spread_halves(rows):
        pieces = lax.optimization_barrier(split(rows))
        chains = [spread(piece) for piece in pieces]
        return [[chain[step] for chain in chains] for step in range(ring)]

    def in_order(blocks):
        first = blocks[0][0]
        whole = jnp.zeros((ring * local_rows,) + first.shape[1:], first.dtype)
        for step, pieces in enumerate(blocks):
            for half, piece in enumerate(pieces):
                whole = lax.dynamic_update_slice_in_dim(
                    whole, piece, block_start_of(step) + half * half_rows, 0
                )
        return whole

    def halves_of(whole, step):
        return [
            lax.dynamic_slice_in_dim(whole, block_start_of(step) + half * half_rows, half_rows, 0)
            for half in range(halves)
        ]

    def collect(parts):
        total = parts[1 % ring].astype(f32)
        for step in range(2, ring + 1):
            total = shift(total.astype(bf16)).astype(f32) + parts[step % ring]
        return total

    def collect_halves(parts):
        return jnp.concatenate(
            [collect([pieces[half] for pieces in parts]) for half in range(halves)],
            axis=0,
        )

    w_qkv_local = jnp.concatenate([w_query[0], w_keyval[0].reshape(w_keyval.shape[1], -1)], axis=1)
    w_qkv_local = row_major(w_qkv_local)
    w_mlp_local = jnp.stack([w_gate_up[0, :, 0], w_gate_up[0, :, 1], jnp.swapaxes(w_down[0], 0, 1)])
    w_qkv = row_major(lax.all_gather(w_qkv_local, "fsdp", axis=0, tiled=True))
    gains_all = lax.all_gather(norm_gains[0], "fsdp", axis=1, tiled=True)
    w_out_all = lax.all_gather(w_attn_out[0], "fsdp", axis=1, tiled=True)
    w_mlp = lax.all_gather(w_mlp_local, "fsdp", axis=1, tiled=True)

    cosine, sine_table = rope_tables(doc_row, head_size)
    block_starts = list(range(0, row_count, block_rows))
    windows = [
        (max(0, start - MAXLEN), start + block_rows) for start in block_starts
    ]
    mask_list = [
        block_mask(doc_row, start, block_rows, windows[index][0], windows[index][1])
        for index, start in enumerate(block_starts)
    ]

    input_blocks = spread_halves(block_input)
    grad_blocks = spread(after(out_cotangent.astype(bf16), input_blocks[-1]))
    normed_pairs = []
    for pieces in input_blocks:
        normed_pairs.append([norm_apply(piece.astype(f32), gains_all[0]) for piece in pieces])
    residual = block_input.astype(f32)
    inv_attn = norm_apply(residual, gains_all[0])[0]
    normed_all = in_order([[pair[1] for pair in pairs] for pairs in normed_pairs])
    qkv = dot(normed_all, w_qkv)
    query_rows = rotate(
        qkv[:, :query_width].reshape(row_count, kv_local, group_size, head_size),
        cosine, sine_table, 1.0,
    ).astype(bf16)
    keyval = qkv[:, query_width:].reshape(row_count, kv_local, 2 * head_size)
    key_rows = rotate(keyval[..., :head_size], cosine, sine_table, 1.0).astype(bf16)
    value_rows = keyval[..., head_size:].astype(bf16)
    out_list = []
    total_list = []
    for block_index, block_start in enumerate(block_starts):
        key_low, key_high = windows[block_index]
        attend_inputs = (
            query_rows[block_start : block_start + block_rows],
            key_rows[key_low:key_high],
            value_rows[key_low:key_high],
        )
        if block_index > 0:
            attend_inputs = after(attend_inputs, out_list[-1])
        out_block, log_total = attend_block(
            *attend_inputs,
            mask_list[block_index],
            score_scale,
        )
        out_list.append(out_block)
        total_list.append(log_total)
    attended = jnp.concatenate(out_list, axis=0).reshape(row_count, -1)
    middle = residual + collect_halves(
        [[dot(piece, w_out_all) for piece in halves_of(attended, step)] for step in range(ring)],
    )
    inv_mlp, normed_mlp = norm_apply(middle, gains_all[1])

    normed_mlp_blocks = [normed_mlp]
    kept, back_parts, out_parts = (), [], []
    for step in range(ring):
        if step > 0:
            source = normed_mlp_blocks[-1]
            if step > 1:
                source = after(source, back_parts[step - 2])
            normed_mlp_blocks.append(shift(source))
        rows = normed_mlp_blocks[step]
        if step > 0:
            rows = after(rows, back_parts[step - 1])
        *kept, back_part, out_part = mlp_block(
            step, ring, rows, grad_blocks[step], w_mlp, tuple(kept)
        )
        back_parts.append(back_part)
        out_parts.append(out_part)
    right_rows, left_rows = kept
    grad_normed_mlp = collect(back_parts)
    grad_mlp = lax.dot_general(
        left_rows, right_rows, (((1,), (1,)), ((0,), (0,))), preferred_element_type=f32
    ).astype(bf16)
    grad_mlp = lax.psum_scatter(grad_mlp, "fsdp", scatter_dimension=1, tiled=True)
    grad_mlp = grad_mlp.astype(f32)
    grad_down = jnp.swapaxes(grad_mlp[0], 0, 1)
    grad_wgu = jnp.swapaxes(grad_mlp[1:], 0, 1)
    gain_mlp_part = jnp.sum(grad_wgu * w_gate_up[0].astype(f32), axis=(1, 2))
    norm_part, _ = norm_back(middle, inv_mlp, gains_all[1], grad_normed_mlp)
    grad_middle = out_cotangent + norm_part

    middle_blocks = [[block] for block in spread(grad_middle.astype(bf16))]
    do_parts = [
        [dot_nt(piece, w_out_all).astype(bf16) for piece in pieces] for pieces in middle_blocks
    ]
    grad_attended = in_order(do_parts).reshape(row_count, kv_local, group_size, head_size)
    middle_all = in_order(middle_blocks)

    grad_wo = dot_tn(middle_all, attended).astype(bf16)

    out_totals = [after(out_parts[1 % ring], middle_blocks[-1]).astype(bf16)]
    for step in range(2, ring + 1):
        source = out_totals[-1]
        if step == ring:
            source = after(source, (grad_wgu, grad_down, gain_mlp_part))
        out_totals.append((shift(source).astype(f32) + out_parts[step % ring]))
        if step < ring:
            out_totals[-1] = out_totals[-1].astype(bf16)
    output_rows = middle + out_totals[-1]

    attended_heads = attended.reshape(row_count, kv_local, group_size, head_size)
    grad_keys = jnp.zeros((row_count, kv_local, head_size), f32)
    grad_values = jnp.zeros((row_count, kv_local, head_size), f32)
    query_grads = []
    for block_index, block_start in enumerate(block_starts):
        block_stop = block_start + block_rows
        key_low, key_high = windows[block_index]
        grad_out = after(grad_attended[block_start:block_stop], out_totals[block_index])
        grad_query_block, grad_key_part, grad_value_part = attend_back(
            query_rows[block_start:block_stop],
            key_rows[key_low:key_high],
            value_rows[key_low:key_high],
            mask_list[block_index],
            total_list[block_index],
            attended_heads[block_start:block_stop],
            grad_out,
            score_scale,
        )
        query_grads.append(grad_query_block)
        pad_width = ((key_low, row_count - key_high), (0, 0), (0, 0))
        grad_keys = grad_keys + jnp.pad(grad_key_part, pad_width)
        grad_values = grad_values + jnp.pad(grad_value_part, pad_width)
    grad_query = (
        rotate(jnp.concatenate(query_grads, axis=0), cosine, sine_table, -1.0)
        .astype(bf16)
        .reshape(row_count, -1)
    )
    grad_keyval = (
        jnp.concatenate([rotate(grad_keys, cosine, sine_table, -1.0), grad_values], axis=-1)
        .astype(bf16)
        .reshape(row_count, -1)
    )
    grad_qkv = jnp.concatenate([grad_query, grad_keyval], axis=1)
    grad_qkv = after(grad_qkv, out_totals[-2])
    in_parts = [
        [dot_nt(piece, w_qkv) for piece in halves_of(grad_qkv, step)] for step in range(ring)
    ]
    grad_normed = collect_halves(in_parts)
    norm_part, _ = norm_back(residual, inv_attn, gains_all[0], grad_normed)
    grad_rows = grad_middle + norm_part

    grad_wqkv = dot_tn(normed_all, grad_qkv)
    grad_wqkv = grad_wqkv.astype(bf16)
    packed = lax.psum_scatter(
        jnp.concatenate([grad_wqkv, grad_wo], axis=1),
        "fsdp", scatter_dimension=0, tiled=True,
    )
    packed = after(packed, (grad_rows, output_rows)).astype(f32)
    qkv_width = grad_wqkv.shape[1]
    grad_wq = packed[:, :query_width]
    grad_wkv = packed[:, query_width:qkv_width].reshape(-1, kv_local, 2 * head_size)
    grad_wo = jnp.swapaxes(packed[:, qkv_width:], 0, 1)
    gain_attn_part = jnp.sum(packed[:, :qkv_width] * w_qkv_local.astype(f32), axis=1)
    gain_part = jnp.stack([gain_attn_part, gain_mlp_part]) / norm_gains[0].astype(f32)
    gain_total = gain_part
    for distance in range(1, ring):
        gain_total = gain_total + lax.ppermute(
            gain_part, "tensor", [(i, (i + distance) % ring) for i in range(ring)]
        )
    return (
        output_rows,
        grad_rows,
        grad_wq[None],
        grad_wkv[None],
        grad_wo[None],
        grad_wgu[None],
        grad_down[None],
        gain_total[None],
    )


def solution(mesh):
    return jax.shard_map(
        per_device,
        mesh=mesh,
        in_specs=(
            P(("fsdp", "tensor"), None),
            P("fsdp", None),
            P(None, "fsdp", "tensor"),
            P(None, "fsdp", "tensor", None),
            P(None, "tensor", "fsdp"),
            P(None, "fsdp", None, "tensor"),
            P(None, "tensor", "fsdp"),
            P(None, None, "fsdp"),
            P(("fsdp", "tensor"), None),
        ),
        out_specs=(
            P(("fsdp", "tensor"), None),
            P(("fsdp", "tensor"), None),
            P(None, "fsdp", "tensor"),
            P(None, "fsdp", "tensor", None),
            P(None, "tensor", "fsdp"),
            P(None, "fsdp", None, "tensor"),
            P(None, "tensor", "fsdp"),
            P(None, None, "fsdp"),
        ),
        check_vma=False,
    )
```
